32 devices in a mesh: pr: 8 (over y, x, core), pc: 4 (over z).
Axes of the slice: x: 2, y: 2, z: 4, core: 2. Of those that a mesh axis runs over, the one named last changes fastest.
Arguments:
- pair_array: bfloat16 [256, 256, 128], P('pr', 'pc'), may hold values from -6 to 6
- left_weight: bfloat16 [128, 128], replicated, may hold values from -0.5 to 0.5
- right_weight: bfloat16 [128, 128], replicated, may hold values from -0.5 to 0.5
- left_gate: bfloat16 [128, 128], replicated, may hold values from -0.5 to 0.5
- right_gate: bfloat16 [128, 128], replicated, may hold values from -0.5 to 0.5
- mid_gain: float32 [128], replicated, may hold values from 0.25 to 1.75
- out_weight: bfloat16 [128, 128], replicated, may hold values from -0.5 to 0.5
- out_gate: bfloat16 [128, 128], replicated, may hold values from -0.5 to 0.5
Outputs:
- pair_update: bfloat16 [256, 256, 128], P('pr', 'pc')
The draws below stay inside these ranges and needn't reach their ends.
All inputs are finite; a program needn't handle non-finite values.
Results may differ from the reference program's by a relative error of at most 0.012.
Values may be sent and summed in bfloat16 or wider, within the bound.
A program may use at most 128 MiB of HBM per device.

```python
import jax
import jax.numpy as jnp
from jax import lax

RESIDUES = 256
PAIR_WIDTH = 128
MIX_WIDTH = 128


def shard_levels(rng, extent, pieces, least, largest):
    loudness = 1.0
    for axis_at, parts in pieces:
        draws = jax.random.uniform(jax.random.fold_in(jax.random.fold_in(rng, 6), axis_at), (parts,), jnp.float32, least / len(pieces), largest / len(pieces))
        loudness = loudness * jnp.repeat(jnp.exp(draws), extent[axis_at] // parts).reshape((-1,) + (1,) * (len(extent) - 1 - axis_at))
    return loudness


def bell_draw(key, shape, scale, reach, pieces=(), dtype=jnp.bfloat16):
    entries = jax.random.normal(key, shape, jnp.float32) * scale
    if len(pieces) > 0:
        entries = shard_levels(key, shape, pieces, -0.22, 0.18) * entries
    return jnp.clip(entries, min=-reach, max=reach).astype(dtype)


def setup_inputs(seed: int = 0) -> dict:
    keys = jax.random.split(jax.random.key(seed), 9)
    pair_array = bell_draw(keys[0], (RESIDUES, RESIDUES, PAIR_WIDTH), 1.0, 6.0, ((0, 8), (1, 4)))
    left_weight = bell_draw(keys[1], (PAIR_WIDTH, MIX_WIDTH), PAIR_WIDTH ** -0.5, 0.5)
    right_weight = bell_draw(keys[2], (PAIR_WIDTH, MIX_WIDTH), PAIR_WIDTH ** -0.5, 0.5)
    left_gate = bell_draw(keys[3], (PAIR_WIDTH, MIX_WIDTH), PAIR_WIDTH ** -0.5, 0.5)
    right_gate = bell_draw(keys[4], (PAIR_WIDTH, MIX_WIDTH), PAIR_WIDTH ** -0.5, 0.5)
    mid_gain = jnp.clip(1.0 + 0.15 * jax.random.normal(keys[5], (MIX_WIDTH,), jnp.float32), 0.25, 1.75)
    out_weight = bell_draw(keys[6], (MIX_WIDTH, PAIR_WIDTH), MIX_WIDTH ** -0.5, 0.5)
    out_gate = bell_draw(keys[7], (PAIR_WIDTH, PAIR_WIDTH), PAIR_WIDTH ** -0.5, 0.5)
    return {"pair_array": pair_array, "left_weight": left_weight, "right_weight": right_weight, "left_gate": left_gate, "right_gate": right_gate, "mid_gain": mid_gain, "out_weight": out_weight, "out_gate": out_gate}


def unit_channels(values, channel_gain):
    centred = values - lax.optimization_barrier(jnp.mean(values, axis=-1, keepdims=True))
    return centred * lax.rsqrt(lax.optimization_barrier(jnp.mean(centred * centred, axis=-1, keepdims=True)) + 1e-05) * channel_gain

def make_factors(pair_in, left_weight, right_weight, left_gate, right_gate):
    ready = pair_in
    left = jnp.einsum('ijc,cd->ijd', ready.astype(jnp.float32), left_weight.astype(jnp.float32))
    left = left * jax.nn.sigmoid(jnp.einsum('ijc,cd->ijd', ready.astype(jnp.float32), left_gate.astype(jnp.float32)))
    right = jnp.einsum('ijc,cd->ijd', ready.astype(jnp.float32), right_weight.astype(jnp.float32))
    right = right * jax.nn.sigmoid(jnp.einsum('ijc,cd->ijd', ready.astype(jnp.float32), right_gate.astype(jnp.float32)))
    return (ready, left.astype(jnp.bfloat16), right.astype(jnp.bfloat16))

def to_pair(mixed, ready, mid_gain, out_weight, out_gate):
    scaled = unit_channels(mixed.astype(jnp.float32), mid_gain).astype(jnp.bfloat16)
    scaled = lax.optimization_barrier(scaled)
    gate = jax.nn.sigmoid(jnp.einsum('ijc,cd->ijd', ready.astype(jnp.float32), out_gate.astype(jnp.float32)))
    return (jnp.einsum('ijd,dc->ijc', scaled.astype(jnp.float32), out_weight.astype(jnp.float32)) * gate).astype(jnp.bfloat16)

def reference(pair_array, left_weight, right_weight, left_gate, right_gate, mid_gain, out_weight, out_gate):
    ready, left, right = make_factors(pair_array, left_weight, right_weight, left_gate, right_gate)
    left, right = lax.optimization_barrier((left, right))

    def one_channel(pair_of):
        return (jnp.dot(pair_of[0].T, pair_of[1], preferred_element_type=jnp.float32) * RESIDUES ** (-0.5)).astype(jnp.bfloat16)
    mixed = jnp.moveaxis(lax.map(one_channel, (jnp.moveaxis(left, -1, 0), jnp.moveaxis(right, -1, 0))), 0, -1)
    mixed = lax.optimization_barrier(mixed)
    return to_pair(mixed, ready, mid_gain, out_weight, out_gate)
```

```python
import functools

import jax
import jax.numpy as jnp
from jax import lax
from jax.experimental import pallas as pl
from jax.experimental.pallas import tpu as pltpu
from jax.sharding import PartitionSpec as P

MESH = pl.DeviceIdType.MESH
BF16 = jnp.bfloat16
F32 = jnp.float32
LANES = 128
SUB = 16
UF, UP, UE = 16, 8, 16


def unit_channels(values, channel_gain):
    centred = values - jnp.mean(values, axis=-1, keepdims=True)
    return (
        centred
        * lax.rsqrt(jnp.mean(centred * centred, axis=-1, keepdims=True) + 1e-05)
        * channel_gain
    )


def make_factors(pair_in, left_weight, right_weight, left_gate, right_gate):
    left = jnp.einsum("ijc,cd->ijd", pair_in, left_weight, preferred_element_type=F32)
    left = left * jax.nn.sigmoid(
        jnp.einsum("ijc,cd->ijd", pair_in, left_gate, preferred_element_type=F32)
    )
    right = jnp.einsum("ijc,cd->ijd", pair_in, right_weight, preferred_element_type=F32)
    right = right * jax.nn.sigmoid(
        jnp.einsum("ijc,cd->ijd", pair_in, right_gate, preferred_element_type=F32)
    )
    return (pair_in, left.astype(BF16), right.astype(BF16))


def to_pair(mixed, ready, mid_gain, out_weight, out_gate):
    scaled = unit_channels(mixed.astype(F32), mid_gain).astype(BF16)
    scaled = lax.optimization_barrier(scaled)
    gate = jax.nn.sigmoid(jnp.einsum("ijc,cd->ijd", ready, out_gate, preferred_element_type=F32))
    return (
        jnp.einsum("ijd,dc->ijc", scaled, out_weight, preferred_element_type=F32) * gate
    ).astype(BF16)


def plain(
    pair_array, left_weight, right_weight, left_gate, right_gate, mid_gain, out_weight, out_gate
):
    ready, left, right = make_factors(pair_array, left_weight, right_weight, left_gate, right_gate)
    count = pair_array.shape[0] * lax.axis_size("pr")
    left_lines, right_lines = (
        lax.all_to_all(left, "pr", split_axis=2, concat_axis=0, tiled=True),
        lax.all_to_all(right, "pr", split_axis=2, concat_axis=0, tiled=True),
    )
    strip = jnp.einsum(
        "kid,kjd->ijd",
        lax.all_gather(left_lines, "pc", axis=1, tiled=True),
        right_lines,
        preferred_element_type=F32,
    )
    strip = (strip * count ** (-0.5)).astype(BF16)
    mixed = lax.all_to_all(strip, "pr", split_axis=0, concat_axis=2, tiled=True)
    return to_pair(mixed, ready, mid_gain, out_weight, out_gate)


def nt(a, b):
    return lax.dot_general(a, b, (((1,), (1,)), ((), ())), preferred_element_type=F32)


def tn(a, b):
    return lax.dot_general(a, b, (((0,), (0,)), ((), ())), preferred_element_type=F32)


GROUPS = ((0, 0), (0, 1), (1, 0), (1, 1))


def kernel(
    n_p, n_q, x_hbm, lw_hbm, rw_hbm, lg_hbm, rg_hbm, gain_hbm, ow_hbm, og_hbm, out_ref,
    x_ref, lw_ref, rw_ref, lg_ref, rg_ref, gain_ref, ow_ref, og_ref, in_s,
    turn, lsend, rsend, lrecv, rrecv, osend, orecv, gate,
    l_ss, l_rs, r_ss, r_rs, o_ss, o_rs,
):
    p = lax.axis_index("pr")
    q = lax.axis_index("pc")
    zh = q // 2
    zl = q % 2
    me = p * 2 + zl
    n_e = n_p * 2
    per = lsend.shape[1] // SUB
    width = x_ref.shape[1]
    rows = x_ref.shape[0] // 2
    channels = n_e * per
    count = n_p * x_ref.shape[0]

    brought = [
        pltpu.make_async_copy(src, dst, in_s.at[at])
        for at, (src, dst) in enumerate(
            (
                (x_hbm, x_ref), (rw_hbm, rw_ref), (rg_hbm, rg_ref), (lw_hbm, lw_ref),
                (lg_hbm, lg_ref), (og_hbm, og_ref), (ow_hbm, ow_ref), (gain_hbm, gain_ref),
            )
        )
    ]
    for copy in brought:
        copy.start()

    barrier = pltpu.get_barrier_semaphore()
    for dp in range(n_p):
        for dh, dl in GROUPS:
            if (dp, dh, dl) != (0, 0, 0):
                to = (lax.rem(p + dp, n_p), lax.rem(zh + dh, 2) * 2 + lax.rem(zl + dl, 2))
                pl.semaphore_signal(barrier, inc=1, device_id=to, device_id_type=MESH)

    def pair_rows(k):
        return jnp.concatenate([x_ref[k], x_ref[k + rows]], axis=0)

    def factor(w_ref, g_ref, send):
        both = jnp.concatenate([w_ref[...].T, g_ref[...].T], axis=0)

        def step(k, _):
            pr = nt(both, pair_rows(k))
            turn[pl.ds(k, channels, stride=SUB), :] = pr[:channels] * jax.nn.sigmoid(pr[channels:])
            return 0

        lax.fori_loop(0, rows, step, 0, unroll=UF)

        def cast(e, _):
            at = pl.multiple_of(e * per * SUB, per * SUB)
            send[e] = turn[pl.ds(at, per * SUB), :].astype(BF16)
            return 0

        lax.fori_loop(0, n_e, cast, 0, unroll=4)

    def r_copy(dp, dl, arriving=False):
        to_p, to_l = lax.rem(p + dp, n_p), lax.rem(zl + dl, 2)
        return pltpu.make_async_remote_copy(
            src_ref=rsend.at[to_p * 2 + to_l],
            dst_ref=rrecv.at[dl, dp],
            send_sem=r_ss.at[dl, dp],
            recv_sem=r_rs.at[dl, dp],
            device_id=(to_p, zh * 2 + to_l),
            device_id_type=MESH,
        )

    def l_copy(dp, group):
        dh, dl = GROUPS[group]
        to_p, to_l = lax.rem(p + dp, n_p), lax.rem(zl + dl, 2)
        return pltpu.make_async_remote_copy(
            src_ref=lsend.at[to_p * 2 + to_l],
            dst_ref=lrecv.at[group, dp],
            send_sem=l_ss.at[group, dp],
            recv_sem=l_rs.at[group, dp],
            device_id=(to_p, lax.rem(zh + dh, 2) * 2 + to_l),
            device_id_type=MESH,
        )

    for copy in brought:
        copy.wait()
    factor(rw_ref, rg_ref, rsend)
    pl.semaphore_wait(barrier, n_p * n_q - 1)
    for dl in (1, 0):
        for dp in range(n_p):
            if (dp, dl) != (0, 0):
                r_copy(dp, dl).start()
    factor(lw_ref, lg_ref, lsend)
    for group in range(4):
        for dp in range(n_p):
            if (dp, group) != (0, 0):
                l_copy(dp, group).start()
    rrecv[0, 0] = rsend[me]
    lrecv[0, 0] = lsend[me]

    def make_gate(k, _):
        gate[k] = jax.nn.sigmoid(
            jnp.dot(pair_rows(k), og_ref[...], preferred_element_type=F32)
        )
        return 0

    lax.fori_loop(0, rows, make_gate, 0, unroll=4)

    for dl in (1, 0):
        for dp in range(n_p):
            if (dp, dl) != (0, 0):
                r_copy(dp, dl).wait_recv()

    low = lax.broadcasted_iota(jnp.int32, (SUB, LANES), 1) < width

    def o_copy(group, b, dl):
        dh, gl = GROUPS[group]
        z = lax.rem(zh + dh, 2) * 2 + lax.rem(zl + gl, 2)
        to_p, to_l = z * 2 + b, lax.rem(zl + dl, 2)
        away = (to_p != p) if dl == 0 else None
        return away, pltpu.make_async_remote_copy(
            src_ref=osend.at[group, b, dl],
            dst_ref=orecv.at[me],
            send_sem=o_ss.at[group, b, dl],
            recv_sem=o_rs.at[me],
            device_id=(to_p, zh * 2 + to_l),
            device_id_type=MESH,
        )

    for group in range(4):
        for dp in range(n_p):
            if (dp, group) != (0, 0):
                l_copy(dp, group).wait_recv()

        def products(d, _):
            at = pl.ds(pl.multiple_of(d * SUB, SUB), SUB)
            left = lrecv[group, :, at, :].reshape(n_p * SUB, LANES)
            right = [rrecv[dl, :, at, :].reshape(n_p * SUB, LANES) for dl in range(2)]
            sums = tn(left, jnp.concatenate(right, axis=1))
            for dl in range(2):
                acc = sums[:, dl * LANES : (dl + 1) * LANES]
                for b in range(2):
                    top = b * 2 * SUB
                    a0, c0 = acc[top : top + SUB], acc[top + SUB : top + 2 * SUB]
                    b0 = acc[width + top : width + top + SUB]
                    d0 = acc[width + top + SUB : width + top + 2 * SUB]
                    tile = jnp.where(low, a0, d0) + pltpu.roll(
                        jnp.where(low, c0, b0), width, 1
                    )
                    osend[group, b, dl, at, :] = (tile * count ** (-0.5)).astype(BF16)
            return 0

        lax.fori_loop(0, per, products, 0, unroll=UP)
        for b in range(2):
            for dl in (1, 0):
                away, copy = o_copy(group, b, dl)
                if away is None:
                    copy.start()
                else:

                    @pl.when(away)
                    def _():
                        copy.start()

                    @pl.when(jnp.logical_not(away))
                    def _():
                        orecv[me] = osend[group, b, dl]

    gain = jnp.broadcast_to(gain_ref[...], (channels, channels)).T
    for dl in range(2):
        for dp in range(n_p):
            if (dp, dl) != (0, 0):
                r_copy(dp, dl).wait_send()
    for group in range(4):
        for dp in range(n_p):
            if (dp, group) != (0, 0):
                l_copy(dp, group).wait_send()
    for off in range(1, n_e):
        at = lax.rem(me + off, n_e)
        pltpu.make_async_remote_copy(
            src_ref=osend.at[0, 0, 0],
            dst_ref=orecv.at[at],
            send_sem=o_ss.at[0, 0, 0],
            recv_sem=o_rs.at[at],
            device_id=(p, q),
            device_id_type=MESH,
        ).wait_recv()

    def widen(e, _):
        at = pl.multiple_of(e * per * SUB, per * SUB)
        turn[pl.ds(at, per * SUB), :] = orecv[e].astype(F32)
        return 0

    lax.fori_loop(0, n_e, widen, 0, unroll=4)

    def finish(k, _):
        v = turn[pl.ds(k, channels, stride=SUB), :]
        v = v - jnp.mean(v, axis=0, keepdims=True)
        v = v * lax.rsqrt(jnp.mean(v * v, axis=0, keepdims=True) + 1e-05) * gain
        res = (tn(v.astype(BF16), ow_ref[...]) * gate[k]).astype(BF16)
        out_ref[k] = res[:width]
        out_ref[k + rows] = res[width:]
        return 0

    lax.fori_loop(0, rows, finish, 0, unroll=UE)

    for group in range(4):
        for b in range(2):
            for dl in range(2):
                away, copy = o_copy(group, b, dl)
                if away is None:
                    copy.wait_send()
                else:

                    @pl.when(away)
                    def _():
                        copy.wait_send()


def fused(n_p, n_q, pair_array, lw, rw, lg, rg, gain, ow, og):
    channels = lw.shape[1]
    n_e = n_p * 2
    slab = channels // n_e * SUB
    rows = pair_array.shape[0] // 2
    dma = pltpu.SemaphoreType.DMA
    return pl.pallas_call(
        functools.partial(kernel, n_p, n_q),
        out_shape=pltpu.VMEM(pair_array.shape, BF16),
        in_specs=[pl.BlockSpec(memory_space=pltpu.HBM)] * 8,
        out_specs=pl.BlockSpec(memory_space=pltpu.VMEM),
        scratch_shapes=[
            pltpu.VMEM(pair_array.shape, BF16),
            *[pltpu.VMEM(lw.shape, BF16)] * 4,
            pltpu.VMEM((1, channels), F32),
            pltpu.VMEM(ow.shape, BF16),
            pltpu.VMEM(og.shape, BF16),
            dma((8,)),
            pltpu.VMEM((channels * SUB, LANES), F32),
            pltpu.VMEM((n_e, slab, LANES), BF16),
            pltpu.VMEM((n_e, slab, LANES), BF16),
            pltpu.VMEM((4, n_p, slab, LANES), BF16),
            pltpu.VMEM((2, n_p, slab, LANES), BF16),
            pltpu.VMEM((4, 2, 2, slab, LANES), BF16),
            pltpu.VMEM((n_e, slab, LANES), BF16),
            pltpu.VMEM((rows, LANES, channels), F32),
            dma((4, n_p)),
            dma((4, n_p)),
            dma((2, n_p)),
            dma((2, n_p)),
            dma((4, 2, 2)),
            dma((n_e,)),
        ],
        compiler_params=pltpu.CompilerParams(
            collective_id=0, has_side_effects=True, vmem_limit_bytes=33_554_432
        ),
    )(*(
        pltpu.with_memory_space_constraint(a, pltpu.HBM)
        for a in (pair_array, lw, rw, lg, rg, gain.reshape(1, channels), ow, og)
    ))


def solution(mesh):
    n_p, n_q = mesh.shape["pr"], mesh.shape["pc"]

    def on_device(pair_array, lw, *rest):
        first, second, wide = pair_array.shape
        fits = (
            n_q == 4
            and first == 2 * SUB
            and second == 2 * first
            and n_p == 2 * n_q
            and 2 * second == LANES
            and wide == LANES
            and lw.shape[1] == LANES
        )
        if fits:
            return fused(n_p, n_q, pair_array, lw, *rest)
        return plain(pair_array, lw, *rest)

    return jax.shard_map(
        on_device,
        mesh=mesh,
        in_specs=(P("pr", "pc", None), P(), P(), P(), P(), P(), P(), P()),
        out_specs=P("pr", "pc", None),
        check_vma=False,
    )
```

```python
import functools

import jax
import jax.numpy as jnp
from jax import lax
from jax.experimental import pallas as pl
from jax.experimental.pallas import tpu as pltpu
from jax.sharding import PartitionSpec as P

MESH = pl.DeviceIdType.MESH
BF16 = jnp.bfloat16
F32 = jnp.float32
LANES = 128
SUB = 16
UF, UP, UE = 16, 8, 16


def unit_channels(values, channel_gain):
    centred = values - jnp.mean(values, axis=-1, keepdims=True)
    return (
        centred
        * lax.rsqrt(jnp.mean(centred * centred, axis=-1, keepdims=True) + 1e-05)
        * channel_gain
    )


def make_factors(pair_in, left_weight, right_weight, left_gate, right_gate):
    left = jnp.einsum("ijc,cd->ijd", pair_in, left_weight, preferred_element_type=F32)
    left = left * jax.nn.sigmoid(
        jnp.einsum("ijc,cd->ijd", pair_in, left_gate, preferred_element_type=F32)
    )
    right = jnp.einsum("ijc,cd->ijd", pair_in, right_weight, preferred_element_type=F32)
    right = right * jax.nn.sigmoid(
        jnp.einsum("ijc,cd->ijd", pair_in, right_gate, preferred_element_type=F32)
    )
    return (pair_in, left.astype(BF16), right.astype(BF16))


def to_pair(mixed, ready, mid_gain, out_weight, out_gate):
    scaled = unit_channels(mixed.astype(F32), mid_gain).astype(BF16)
    scaled = lax.optimization_barrier(scaled)
    gate = jax.nn.sigmoid(jnp.einsum("ijc,cd->ijd", ready, out_gate, preferred_element_type=F32))
    return (
        jnp.einsum("ijd,dc->ijc", scaled, out_weight, preferred_element_type=F32) * gate
    ).astype(BF16)


def plain(
    pair_array, left_weight, right_weight, left_gate, right_gate, mid_gain, out_weight, out_gate
):
    ready, left, right = make_factors(pair_array, left_weight, right_weight, left_gate, right_gate)
    count = pair_array.shape[0] * lax.axis_size("pr")
    left_lines, right_lines = (
        lax.all_to_all(left, "pr", split_axis=2, concat_axis=0, tiled=True),
        lax.all_to_all(right, "pr", split_axis=2, concat_axis=0, tiled=True),
    )
    strip = jnp.einsum(
        "kid,kjd->ijd",
        lax.all_gather(left_lines, "pc", axis=1, tiled=True),
        right_lines,
        preferred_element_type=F32,
    )
    strip = (strip * count ** (-0.5)).astype(BF16)
    mixed = lax.all_to_all(strip, "pr", split_axis=0, concat_axis=2, tiled=True)
    return to_pair(mixed, ready, mid_gain, out_weight, out_gate)


def nt(a, b):
    return lax.dot_general(a, b, (((1,), (1,)), ((), ())), preferred_element_type=F32)


def tn(a, b):
    return lax.dot_general(a, b, (((0,), (0,)), ((), ())), preferred_element_type=F32)


HOME = (3, 3)
MOVED = (4, 4, 2)
CHUNKS = HOME + MOVED
ORDER = ('M', 'N0', 'N1', 'O', 'g', 'F0', 'N2', 'C0', 'F1', 'N3', 'C1', 'N4', 'F2', 'D0', 'P0', 'Q0', 'C2', 'P2', 'D1', 'P1', 'Q1', 'F3', 'C3', 'P3', 'F4', 'D2', 'Q2', 'C4', 'P4', 'D3', 'Q3', 'D4', 'Q4')


def kernel(
    n_p, n_q, x_hbm, lw_hbm, rw_hbm, lg_hbm, rg_hbm, gain_hbm, ow_hbm, og_hbm, out_ref,
    x_ref, lw_ref, rw_ref, lg_ref, rg_ref, gain_ref, ow_ref, og_ref, in_s,
    turn, lsend, rsend, lbuf, rbuf, osend, orecv, gate,
    a_ss, a_rs, f_ss, own_rs, f_rs, e_ss, e_rs, o_ss, o_rs,
):
    p = lax.axis_index("pr")
    q = lax.axis_index("pc")
    half = q // 2
    mid, end = 1 + half, 3 * half
    far_mid, far_end = 2 - half, 3 - 3 * half
    at_mid = q == mid
    per = lsend.shape[1] // SUB
    width = x_ref.shape[1]
    rows = x_ref.shape[0] // 2
    channels = n_p * per
    count = n_p * x_ref.shape[0]
    planes = (mid, end, far_mid, far_end)
    n_c = len(CHUNKS)
    part = [pl.ds(sum(CHUNKS[:c]) * SUB, CHUNKS[c] * SUB) for c in range(n_c)]
    others = pl.ds(1, n_p - 1)
    pair = pl.ds(0, 2)
    away = pl.ds(2, n_p - 2)
    n_h = len(HOME)
    home = pl.ds(0, sum(HOME) * SUB)
    moved = pl.ds(sum(HOME) * SUB, sum(MOVED) * SUB)

    brought = [
        pltpu.make_async_copy(src, dst, in_s.at[at])
        for at, (src, dst) in enumerate(
            (
                (x_hbm, x_ref), (lw_hbm, lw_ref), (lg_hbm, lg_ref), (rw_hbm, rw_ref),
                (rg_hbm, rg_ref), (og_hbm, og_ref), (ow_hbm, ow_ref), (gain_hbm, gain_ref),
            )
        )
    ]
    for copy in brought:
        copy.start()

    barrier = pltpu.get_barrier_semaphore()
    for dp in range(n_p):
        for dq in range(n_q):
            if (dp, dq) != (0, 0):
                pl.semaphore_signal(
                    barrier, inc=1, device_id=(p ^ dp, q ^ dq), device_id_type=MESH
                )

    def pair_rows(k):
        return jnp.concatenate([x_ref[k], x_ref[k + rows]], axis=0)

    def factor(w_ref, g_ref, send):
        both = jnp.concatenate([w_ref[...].T, g_ref[...].T], axis=0)

        def step(k, _):
            pr = nt(both, pair_rows(k))
            turn[pl.ds(k, channels, stride=SUB), :] = pr[:channels] * jax.nn.sigmoid(pr[channels:])
            return 0

        lax.fori_loop(0, rows, step, 0, unroll=UF)

        def cast(e, _):
            at = pl.multiple_of(e * per * SUB, per * SUB)
            send[e] = turn[pl.ds(at, per * SUB), :].astype(BF16)
            return 0

        lax.fori_loop(0, n_p, cast, 0, unroll=2)

    def remote(src, dst, send_sem, recv_sem, to):
        return pltpu.make_async_remote_copy(
            src_ref=src, dst_ref=dst, send_sem=send_sem, recv_sem=recv_sem,
            device_id=to, device_id_type=MESH,
        )

    def arrived(ref, sem):
        remote(ref, ref, sem, sem, (p, q)).wait_recv()

    def left(ref, sem):
        remote(ref, ref, sem, sem, (p, q)).wait_send()

    def spread(kind, send, buf, order):
        def give(dp, lines, at):
            remote(
                send.at[p ^ dp, lines], buf.at[0, dp, lines],
                a_ss.at[kind], a_rs.at[kind, at], (p ^ dp, q),
            ).start()

        give(1, slice(None), n_c)
        for c in order:
            for dp in range(n_p - 1, 1, -1):
                give(dp, part[c], c)

    def own(buf, slot_from, slot_to, at, to, slots, lines=slice(None), sem=None):
        remote(
            buf.at[slot_from, slots, lines], buf.at[slot_to, slots, lines],
            f_ss.at[at], own_rs.at[at if sem is None else sem], to,
        ).start()

    def pass_on(buf, slot_from, slot_to, at, c, to):
        remote(
            buf.at[slot_from, away, part[c]], buf.at[slot_to, away, part[c]],
            f_ss.at[at], f_rs.at[at, c], to,
        ).start()

    def to_end(slot_from, slot_to, c):
        remote(
            lbuf.at[slot_from, :, part[c]], lbuf.at[slot_to, :, part[c]],
            e_ss, e_rs.at[slot_to, c], (p, end),
        ).start()

    for copy in brought:
        copy.wait()
    factor(lw_ref, lg_ref, lsend)
    pl.semaphore_wait(barrier, n_p * n_q - 1)
    spread(0, lsend, lbuf, range(n_c))
    lbuf[0, 0] = lsend[p]

    @pl.when(at_mid)
    def _():
        own(lbuf, 0, 2, 2, (p, far_mid), 0)

    @pl.when(jnp.logical_not(at_mid))
    def _():
        own(lbuf, 0, 1, 0, (p, mid), 0)

    factor(rw_ref, rg_ref, rsend)
    rbuf[0, 0] = rsend[p]
    spread(1, rsend, rbuf, (*range(n_h, n_c), *range(n_h)))

    def make_gate(k, _):
        gate[k] = jax.nn.sigmoid(
            jnp.dot(pair_rows(k), og_ref[...], preferred_element_type=F32)
        )
        return 0

    def gates():
        lax.fori_loop(0, rows, make_gate, 0, unroll=4)

    low = lax.broadcasted_iota(jnp.int32, (SUB, LANES), 1) < width

    def multiply(g, c, plane, sides):
        def products(d, _):
            at = pl.ds(pl.multiple_of(d * SUB, SUB), SUB)
            lines = lbuf[g, :, at, :].reshape(n_p * SUB, LANES)
            right = [rbuf[j, :, at, :].reshape(n_p * SUB, LANES) for j in range(sides)]
            sums = tn(lines, right[0] if sides == 1 else jnp.concatenate(right, axis=1))
            for j in range(sides):
                acc = sums[:, j * LANES : (j + 1) * LANES]
                for b in range(2):
                    top = b * 2 * SUB
                    a0, c0 = acc[top : top + SUB], acc[top + SUB : top + 2 * SUB]
                    b0 = acc[width + top : width + top + SUB]
                    d0 = acc[width + top + SUB : width + top + 2 * SUB]
                    tile = jnp.where(low, a0, d0) + pltpu.roll(
                        jnp.where(low, c0, b0), width, 1
                    )
                    osend[g, b, j, at, :] = (tile * count ** (-0.5)).astype(BF16)
            return 0

        first = sum(CHUNKS[:c])
        lax.fori_loop(first, first + CHUNKS[c], products, 0, unroll=CHUNKS[c])
        done = o_rs.at[0 if c < n_h else 1]
        for b in range(2):
            to_p = plane * 2 + b
            if sides == 2:
                remote(
                    osend.at[g, b, 1, part[c]], orecv.at[p, part[c]],
                    o_ss.at[1], done, (to_p, end),
                ).start()

            @pl.when(to_p != p)
            def _():
                remote(
                    osend.at[g, b, 0, part[c]], orecv.at[p, part[c]],
                    o_ss.at[0], done, (to_p, q),
                ).start()

            @pl.when(to_p == p)
            def _():
                orecv[p, part[c]] = osend[g, b, 0, part[c]]

    turn_of = p // 2

    def rotated(n, c, plane_of, sides):
        for t in range(n):
            g = lax.rem(turn_of + t, n)
            plane = plane_of[n - 1]
            for at in range(n - 1):
                plane = jnp.where(g == at, plane_of[at], plane)
            multiply(g, c, plane, sides)

    @pl.when(jnp.logical_not(at_mid))
    def _():
        def pass_left(c):
            arrived(lbuf.at[0, away, part[c]], a_rs.at[0, c])
            pass_on(lbuf, 0, 1, 0, c, (p, mid))

        def pass_right(c):
            arrived(rbuf.at[0, away, part[c]], a_rs.at[1, c])
            pass_on(rbuf, 0, 1, 1, c, (p, mid))

        arrived(lbuf.at[0, 1], a_rs.at[0, n_c])
        own(lbuf, 0, 1, 0, (p, mid), 1, sem=4)
        pass_left(0)
        arrived(rbuf.at[0, 1], a_rs.at[1, n_c])
        for c in range(1, n_h):
            pass_left(c)
        own(rbuf, 0, 1, 1, (p, mid), pair, moved)
        pass_left(n_h)
        for c in range(n_h, n_c):
            pass_right(c)
            if c + 1 < n_c:
                pass_left(c + 1)
        gates()
        for c in range(n_h):
            arrived(rbuf.at[0, away, part[c]], a_rs.at[1, c])
            arrived(lbuf.at[1, :, part[c]], e_rs.at[1, c])
            arrived(lbuf.at[2, :, part[c]], e_rs.at[2, c])
            rotated(3, c, (end, mid, far_mid), 1)
        for c in range(n_h):
            arrived(lbuf.at[3, :, part[c]], e_rs.at[3, c])
            multiply(3, c, far_end, 1)
        left(lbuf.at[0], f_ss.at[0])
        left(lbuf.at[0, :, moved], f_ss.at[1])

    @pl.when(at_mid)
    def _():
        def pass_near(c):
            arrived(lbuf.at[0, away, part[c]], a_rs.at[0, c])
            pass_on(lbuf, 0, 2, 2, c, (p, far_mid))
            if c < n_h:
                to_end(0, 1, c)

        def pass_far(c):
            arrived(lbuf.at[1, away, part[c]], f_rs.at[0, c])
            pass_on(lbuf, 1, 3, 3, c, (p, far_mid))

        def came(c):
            if c == 0:
                arrived(lbuf.at[2, 0], own_rs.at[2])
                arrived(lbuf.at[2, 1], own_rs.at[5])
            arrived(lbuf.at[2, away, part[c]], f_rs.at[2, c])
            if c < n_h:
                to_end(2, 2, c)

        def near(c):
            if c == n_h:
                arrived(rbuf.at[1, pair, moved], own_rs.at[1])
            arrived(rbuf.at[0, away, part[c]], a_rs.at[1, c])
            if c >= n_h:
                arrived(rbuf.at[1, away, part[c]], f_rs.at[1, c])
            rotated(3, c, planes[:3], 1 if c < n_h else 2)

        def mate():
            arrived(lbuf.at[0, 1], a_rs.at[0, n_c])
            own(lbuf, 0, 2, 2, (p, far_mid), 1, sem=5)

        def onward():
            arrived(lbuf.at[1, 0], own_rs.at[0])
            arrived(lbuf.at[1, 1], own_rs.at[4])
            own(lbuf, 1, 3, 3, (p, far_mid), pair)

        def came_far(c):
            if c == 0:
                arrived(lbuf.at[3, pair], own_rs.at[3])
            arrived(lbuf.at[3, away, part[c]], f_rs.at[3, c])
            if c < n_h:
                to_end(3, 3, c)

        def last(c):
            multiply(3, c, far_end, 1 if c < n_h else 2)

        first_right = next(step for step in ORDER if step[0] == "P")
        act = {"N": pass_near, "F": pass_far, "C": came, "P": near, "D": came_far, "Q": last}
        alone = {"M": mate, "O": onward, "g": gates}
        for step in ORDER:
            if step == first_right:
                arrived(rbuf.at[0, 1], a_rs.at[1, n_c])
            if step in alone:
                alone[step]()
            else:
                act[step[0]](int(step[1:]))
        left(lbuf.at[0], f_ss.at[2])
        left(lbuf.at[0], f_ss.at[3])
        left(lbuf.at[pl.ds(1, 3), :, home], e_ss)

    gain = jnp.broadcast_to(gain_ref[...], (channels, channels)).T
    left(lbuf.at[0, others], a_ss.at[0])
    left(lbuf.at[0, others], a_ss.at[1])

    arrived(orecv.at[others, home], o_rs.at[0])

    @pl.when(at_mid)
    def _():
        arrived(orecv.at[others, moved], o_rs.at[1])

    @pl.when(jnp.logical_not(at_mid))
    def _():
        arrived(orecv.at[:, moved], o_rs.at[1])

    def widen(e, _):
        at = pl.multiple_of(e * per * SUB, per * SUB)
        turn[pl.ds(at, per * SUB), :] = orecv[e].astype(F32)
        return 0

    lax.fori_loop(0, n_p, widen, 0, unroll=2)

    def finish(k, _):
        v = turn[pl.ds(k, channels, stride=SUB), :]
        v = v - jnp.mean(v, axis=0, keepdims=True)
        v = v * lax.rsqrt(jnp.mean(v * v, axis=0, keepdims=True) + 1e-05) * gain
        res = (tn(v.astype(BF16), ow_ref[...]) * gate[k]).astype(BF16)
        out_ref[k] = res[:width]
        out_ref[k + rows] = res[width:]
        return 0

    lax.fori_loop(0, rows, finish, 0, unroll=UE)

    left(orecv.at[others, home], o_ss.at[0])

    @pl.when(at_mid)
    def _():
        left(orecv.at[others, moved], o_ss.at[0])
        left(orecv.at[:, moved], o_ss.at[1])


def fused(n_p, n_q, pair_array, lw, rw, lg, rg, gain, ow, og):
    channels = lw.shape[1]
    slab = channels // n_p * SUB
    rows = pair_array.shape[0] // 2
    dma = pltpu.SemaphoreType.DMA
    return pl.pallas_call(
        functools.partial(kernel, n_p, n_q),
        out_shape=pltpu.VMEM(pair_array.shape, BF16),
        in_specs=[pl.BlockSpec(memory_space=pltpu.HBM)] * 8,
        out_specs=pl.BlockSpec(memory_space=pltpu.VMEM),
        scratch_shapes=[
            pltpu.VMEM(pair_array.shape, BF16),
            *[pltpu.VMEM(lw.shape, BF16)] * 4,
            pltpu.VMEM((1, channels), F32),
            pltpu.VMEM(ow.shape, BF16),
            pltpu.VMEM(og.shape, BF16),
            dma((8,)),
            pltpu.VMEM((channels * SUB, LANES), F32),
            pltpu.VMEM((n_p, slab, LANES), BF16),
            pltpu.VMEM((n_p, slab, LANES), BF16),
            pltpu.VMEM((4, n_p, slab, LANES), BF16),
            pltpu.VMEM((2, n_p, slab, LANES), BF16),
            pltpu.VMEM((4, 2, 2, slab, LANES), BF16),
            pltpu.VMEM((n_p, slab, LANES), BF16),
            pltpu.VMEM((rows, LANES, channels), F32),
            dma((2,)),
            dma((2, len(CHUNKS) + 1)),
            dma((4,)),
            dma((6,)),
            dma((4, len(CHUNKS))),
            dma(()),
            dma((4, len(HOME))),
            dma((2,)),
            dma((2,)),
        ],
        compiler_params=pltpu.CompilerParams(
            collective_id=0, has_side_effects=True, vmem_limit_bytes=33_554_432
        ),
    )(*(
        pltpu.with_memory_space_constraint(a, pltpu.HBM)
        for a in (pair_array, lw, rw, lg, rg, gain.reshape(1, channels), ow, og)
    ))


def solution(mesh):
    n_p, n_q = mesh.shape["pr"], mesh.shape["pc"]

    def on_device(pair_array, lw, *rest):
        first, second, wide = pair_array.shape
        fits = (
            n_q == 4
            and first == 2 * SUB
            and second == 2 * first
            and n_p == 2 * n_q
            and 2 * second == LANES
            and wide == LANES
            and lw.shape[1] == LANES
            and n_p * sum(CHUNKS) == LANES
        )
        if fits:
            return fused(n_p, n_q, pair_array, lw, *rest)
        return plain(pair_array, lw, *rest)

    return jax.shard_map(
        on_device,
        mesh=mesh,
        in_specs=(P("pr", "pc", None), P(), P(), P(), P(), P(), P(), P()),
        out_specs=P("pr", "pc", None),
        check_vma=False,
    )
```

```python
import functools

import jax
import jax.numpy as jnp
from jax import lax
from jax.experimental import pallas as pl
from jax.experimental.pallas import tpu as pltpu
from jax.sharding import PartitionSpec as P

MESH = pl.DeviceIdType.MESH
BF16 = jnp.bfloat16
F32 = jnp.float32
LANES = 128
SUB = 16
UF, UP, UE = 16, 8, 16


def unit_channels(values, channel_gain):
    centred = values - jnp.mean(values, axis=-1, keepdims=True)
    return (
        centred
        * lax.rsqrt(jnp.mean(centred * centred, axis=-1, keepdims=True) + 1e-05)
        * channel_gain
    )


def make_factors(pair_in, left_weight, right_weight, left_gate, right_gate):
    left = jnp.einsum("ijc,cd->ijd", pair_in, left_weight, preferred_element_type=F32)
    left = left * jax.nn.sigmoid(
        jnp.einsum("ijc,cd->ijd", pair_in, left_gate, preferred_element_type=F32)
    )
    right = jnp.einsum("ijc,cd->ijd", pair_in, right_weight, preferred_element_type=F32)
    right = right * jax.nn.sigmoid(
        jnp.einsum("ijc,cd->ijd", pair_in, right_gate, preferred_element_type=F32)
    )
    return (pair_in, left.astype(BF16), right.astype(BF16))


def to_pair(mixed, ready, mid_gain, out_weight, out_gate):
    scaled = unit_channels(mixed.astype(F32), mid_gain).astype(BF16)
    scaled = lax.optimization_barrier(scaled)
    gate = jax.nn.sigmoid(jnp.einsum("ijc,cd->ijd", ready, out_gate, preferred_element_type=F32))
    return (
        jnp.einsum("ijd,dc->ijc", scaled, out_weight, preferred_element_type=F32) * gate
    ).astype(BF16)


def plain(
    pair_array, left_weight, right_weight, left_gate, right_gate, mid_gain, out_weight, out_gate
):
    ready, left, right = make_factors(pair_array, left_weight, right_weight, left_gate, right_gate)
    count = pair_array.shape[0] * lax.axis_size("pr")
    left_lines, right_lines = (
        lax.all_to_all(left, "pr", split_axis=2, concat_axis=0, tiled=True),
        lax.all_to_all(right, "pr", split_axis=2, concat_axis=0, tiled=True),
    )
    strip = jnp.einsum(
        "kid,kjd->ijd",
        lax.all_gather(left_lines, "pc", axis=1, tiled=True),
        right_lines,
        preferred_element_type=F32,
    )
    strip = (strip * count ** (-0.5)).astype(BF16)
    mixed = lax.all_to_all(strip, "pr", split_axis=0, concat_axis=2, tiled=True)
    return to_pair(mixed, ready, mid_gain, out_weight, out_gate)


def nt(a, b):
    return lax.dot_general(a, b, (((1,), (1,)), ((), ())), preferred_element_type=F32)


def tn(a, b):
    return lax.dot_general(a, b, (((0,), (0,)), ((), ())), preferred_element_type=F32)


HOME = (3, 3)
MOVED = (4, 4, 2)
CHUNKS = HOME + MOVED
ORDER = ('M', 'N0', 'N1', 'O', 'T0', 'T1', 'g', 'F0', 'N2', 'C0', 'F1', 'N3', 'C1', 'N4', 'F2', 'D0', 'P0', 'Q0', 'P2', 'C2', 'G2', 'D1', 'P1', 'Q1', 'F3', 'P3', 'C3', 'G3', 'F4', 'P4', 'D2', 'Q2', 'C4', 'G4', 'D3', 'Q3', 'D4', 'Q4')
END_ORDER = ('L0', 'L1', 'B', 'L2', 'R2', 'L3', 'R3', 'L4', 'R4')
WHOLE = tuple(c for c in range(len(CHUNKS)) if f"G{c}" not in ORDER)


def kernel(
    n_p, n_q, x_hbm, lw_hbm, rw_hbm, lg_hbm, rg_hbm, gain_hbm, ow_hbm, og_hbm, out_ref,
    x_ref, lw_ref, rw_ref, lg_ref, rg_ref, gain_ref, ow_ref, og_ref, in_s,
    turn, lsend, rsend, lbuf, rbuf, osend, orecv, gate,
    a_ss, a_rs, f_ss, own_rs, f_rs, e_ss, e_rs, o_ss, o_rs,
):
    p = lax.axis_index("pr")
    q = lax.axis_index("pc")
    half = q // 2
    mid, end = 1 + half, 3 * half
    far_mid, far_end = 2 - half, 3 - 3 * half
    at_mid = q == mid
    per = lsend.shape[1] // SUB
    width = x_ref.shape[1]
    rows = x_ref.shape[0] // 2
    channels = n_p * per
    count = n_p * x_ref.shape[0]
    planes = (mid, end, far_mid, far_end)
    n_c = len(CHUNKS)
    part = [pl.ds(sum(CHUNKS[:c]) * SUB, CHUNKS[c] * SUB) for c in range(n_c)]
    others = pl.ds(1, n_p - 1)
    pair = pl.ds(0, 2)
    away = pl.ds(2, n_p - 2)
    n_h = len(HOME)
    home = pl.ds(0, sum(HOME) * SUB)
    moved = pl.ds(sum(HOME) * SUB, sum(MOVED) * SUB)

    brought = [
        pltpu.make_async_copy(src, dst, in_s.at[at])
        for at, (src, dst) in enumerate(
            (
                (x_hbm, x_ref), (lw_hbm, lw_ref), (lg_hbm, lg_ref), (rw_hbm, rw_ref),
                (rg_hbm, rg_ref), (og_hbm, og_ref), (ow_hbm, ow_ref), (gain_hbm, gain_ref),
            )
        )
    ]
    for copy in brought:
        copy.start()

    barrier = pltpu.get_barrier_semaphore()
    def greet(to):
        pl.semaphore_signal(barrier, inc=1, device_id=to, device_id_type=MESH)

    for dp in range(1, n_p):
        greet((p ^ dp, q))

    @pl.when(at_mid)
    def _():
        greet((p, far_mid))
        greet((p, end))


    def pair_rows(k):
        return jnp.concatenate([x_ref[k], x_ref[k + rows]], axis=0)

    def factor(w_ref, g_ref, send):
        both = jnp.concatenate([w_ref[...].T, g_ref[...].T], axis=0)

        def step(k, _):
            pr = nt(both, pair_rows(k))
            turn[pl.ds(k, channels, stride=SUB), :] = pr[:channels] * jax.nn.sigmoid(pr[channels:])
            return 0

        lax.fori_loop(0, rows, step, 0, unroll=UF)

        def cast(e, _):
            at = pl.multiple_of(e * per * SUB, per * SUB)
            send[e] = turn[pl.ds(at, per * SUB), :].astype(BF16)
            return 0

        lax.fori_loop(0, n_p, cast, 0, unroll=2)

    def remote(src, dst, send_sem, recv_sem, to):
        return pltpu.make_async_remote_copy(
            src_ref=src, dst_ref=dst, send_sem=send_sem, recv_sem=recv_sem,
            device_id=to, device_id_type=MESH,
        )

    def arrived(ref, sem):
        remote(ref, ref, sem, sem, (p, q)).wait_recv()

    def left(ref, sem):
        remote(ref, ref, sem, sem, (p, q)).wait_send()

    def spread(kind, send, buf, order):
        def give(dp, lines, at):
            remote(
                send.at[p ^ dp, lines], buf.at[0, dp, lines],
                a_ss.at[kind], a_rs.at[kind, at], (p ^ dp, q),
            ).start()

        give(1, slice(None), n_c)
        for c in order:
            for dp in range(n_p - 1, 1, -1):
                give(dp, part[c], c)

    def own(buf, slot_from, slot_to, at, to, slots, lines=slice(None), sem=None):
        remote(
            buf.at[slot_from, slots, lines], buf.at[slot_to, slots, lines],
            f_ss.at[at], own_rs.at[at if sem is None else sem], to,
        ).start()

    def pass_on(buf, slot_from, slot_to, at, c, to):
        remote(
            buf.at[slot_from, away, part[c]], buf.at[slot_to, away, part[c]],
            f_ss.at[at], f_rs.at[at, c], to,
        ).start()

    def to_end(slot_from, slot_to, c):
        remote(
            lbuf.at[slot_from, :, part[c]], lbuf.at[slot_to, :, part[c]],
            e_ss, e_rs.at[slot_to, c], (p, end),
        ).start()

    for copy in brought:
        copy.wait()
    factor(lw_ref, lg_ref, lsend)
    pl.semaphore_wait(barrier, n_p)
    spread(0, lsend, lbuf, range(n_c))
    lbuf[0, 0] = lsend[p]

    @pl.when(at_mid)
    def _():
        own(lbuf, 0, 2, 2, (p, far_mid), 0)

    @pl.when(jnp.logical_not(at_mid))
    def _():
        own(lbuf, 0, 1, 0, (p, mid), 0)

    factor(rw_ref, rg_ref, rsend)
    rbuf[0, 0] = rsend[p]
    spread(1, rsend, rbuf, (*range(n_h, n_c), *range(n_h)))

    def make_gate(k, _):
        gate[k] = jax.nn.sigmoid(
            jnp.dot(pair_rows(k), og_ref[...], preferred_element_type=F32)
        )
        return 0

    def gates():
        lax.fori_loop(0, rows, make_gate, 0, unroll=4)

    low = lax.broadcasted_iota(jnp.int32, (SUB, LANES), 1) < width

    def multiply(g, c, plane, sides):
        def products(d, _):
            at = pl.ds(pl.multiple_of(d * SUB, SUB), SUB)
            lines = lbuf[g, :, at, :].reshape(n_p * SUB, LANES)
            right = [rbuf[j, :, at, :].reshape(n_p * SUB, LANES) for j in range(sides)]
            sums = tn(lines, right[0] if sides == 1 else jnp.concatenate(right, axis=1))
            for j in range(sides):
                acc = sums[:, j * LANES : (j + 1) * LANES]
                for b in range(2):
                    top = b * 2 * SUB
                    a0, c0 = acc[top : top + SUB], acc[top + SUB : top + 2 * SUB]
                    b0 = acc[width + top : width + top + SUB]
                    d0 = acc[width + top + SUB : width + top + 2 * SUB]
                    tile = jnp.where(low, a0, d0) + pltpu.roll(
                        jnp.where(low, c0, b0), width, 1
                    )
                    osend[g, b, j, at, :] = (tile * count ** (-0.5)).astype(BF16)
            return 0

        first = sum(CHUNKS[:c])
        lax.fori_loop(first, first + CHUNKS[c], products, 0, unroll=CHUNKS[c])
        done = o_rs.at[0 if c < n_h else 1]
        for b in range(2):
            to_p = plane * 2 + b
            if sides == 2:
                remote(
                    osend.at[g, b, 1, part[c]], orecv.at[p, part[c]],
                    o_ss.at[1], done, (to_p, end),
                ).start()

            @pl.when(to_p != p)
            def _():
                remote(
                    osend.at[g, b, 0, part[c]], orecv.at[p, part[c]],
                    o_ss.at[0], done, (to_p, q),
                ).start()

            @pl.when(to_p == p)
            def _():
                orecv[p, part[c]] = osend[g, b, 0, part[c]]

    turn_of = p // 2

    def rotated(n, c, plane_of, sides):
        for t in range(n):
            g = lax.rem(turn_of + t, n)
            plane = plane_of[n - 1]
            for at in range(n - 1):
                plane = jnp.where(g == at, plane_of[at], plane)
            multiply(g, c, plane, sides)

    @pl.when(jnp.logical_not(at_mid))
    def _():
        def pass_left(c):
            arrived(lbuf.at[0, away, part[c]], a_rs.at[0, c])
            pass_on(lbuf, 0, 1, 0, c, (p, mid))

        def pass_right(c):
            arrived(rbuf.at[0, away, part[c]], a_rs.at[1, c])
            pass_on(rbuf, 0, 1, 1, c, (p, mid))

        arrived(lbuf.at[0, 1], a_rs.at[0, n_c])
        own(lbuf, 0, 1, 0, (p, mid), 1, sem=4)

        def right_pair():
            arrived(rbuf.at[0, 1], a_rs.at[1, n_c])
            own(rbuf, 0, 1, 1, (p, mid), pair, moved)

        for step in END_ORDER:
            if step == "B":
                right_pair()
            else:
                {"L": pass_left, "R": pass_right}[step[0]](int(step[1:]))
        gates()
        for c in range(n_h):
            arrived(rbuf.at[0, away, part[c]], a_rs.at[1, c])
            arrived(lbuf.at[1, :, part[c]], e_rs.at[1, c])
            arrived(lbuf.at[2, :, part[c]], e_rs.at[2, c])
            rotated(3, c, (end, mid, far_mid), 1)
        for c in range(n_h):
            arrived(lbuf.at[3, :, part[c]], e_rs.at[3, c])
            multiply(3, c, far_end, 1)
        left(lbuf.at[0], f_ss.at[0])
        left(lbuf.at[0, :, moved], f_ss.at[1])

    @pl.when(at_mid)
    def _():
        def pass_near(c):
            arrived(lbuf.at[0, away, part[c]], a_rs.at[0, c])
            pass_on(lbuf, 0, 2, 2, c, (p, far_mid))

        def pass_far(c):
            arrived(lbuf.at[1, away, part[c]], f_rs.at[0, c])
            pass_on(lbuf, 1, 3, 3, c, (p, far_mid))

        def came(c):
            if c == 0:
                arrived(lbuf.at[2, 0], own_rs.at[2])
                arrived(lbuf.at[2, 1], own_rs.at[5])
            arrived(lbuf.at[2, away, part[c]], f_rs.at[2, c])
            if c < n_h:
                to_end(2, 2, c)

        def near(c):
            if c == n_h:
                arrived(rbuf.at[1, pair, moved], own_rs.at[1])
            arrived(rbuf.at[0, away, part[c]], a_rs.at[1, c])
            if c >= n_h:
                arrived(rbuf.at[1, away, part[c]], f_rs.at[1, c])
            rotated(3 if c in WHOLE else 2, c, planes, 1 if c < n_h else 2)

        def near_to_end(c):
            to_end(0, 1, c)

        def far_near(c):
            multiply(2, c, far_mid, 1 if c < n_h else 2)

        def mate():
            arrived(lbuf.at[0, 1], a_rs.at[0, n_c])
            own(lbuf, 0, 2, 2, (p, far_mid), 1, sem=5)

        def onward():
            arrived(lbuf.at[1, 0], own_rs.at[0])
            arrived(lbuf.at[1, 1], own_rs.at[4])
            own(lbuf, 1, 3, 3, (p, far_mid), pair)

        def came_far(c):
            if c == 0:
                arrived(lbuf.at[3, pair], own_rs.at[3])
            arrived(lbuf.at[3, away, part[c]], f_rs.at[3, c])
            if c < n_h:
                to_end(3, 3, c)

        def last(c):
            multiply(3, c, far_end, 1 if c < n_h else 2)

        first_right = next(step for step in ORDER if step[0] == "P")
        act = {"N": pass_near, "F": pass_far, "C": came, "P": near, "G": far_near, "T": near_to_end, "D": came_far, "Q": last}
        alone = {"M": mate, "O": onward, "g": gates}
        for step in ORDER:
            if step == first_right:
                arrived(rbuf.at[0, 1], a_rs.at[1, n_c])
            if step in alone:
                alone[step]()
            else:
                act[step[0]](int(step[1:]))
        left(lbuf.at[0], f_ss.at[2])
        left(lbuf.at[0], f_ss.at[3])
        left(lbuf.at[pl.ds(1, 3), :, home], e_ss)

    gain = jnp.broadcast_to(gain_ref[...], (channels, channels)).T
    left(lbuf.at[0, others], a_ss.at[0])
    left(lbuf.at[0, others], a_ss.at[1])

    arrived(orecv.at[others, home], o_rs.at[0])

    @pl.when(at_mid)
    def _():
        arrived(orecv.at[others, moved], o_rs.at[1])

    @pl.when(jnp.logical_not(at_mid))
    def _():
        arrived(orecv.at[:, moved], o_rs.at[1])

    def widen(e, _):
        at = pl.multiple_of(e * per * SUB, per * SUB)
        turn[pl.ds(at, per * SUB), :] = orecv[e].astype(F32)
        return 0

    lax.fori_loop(0, n_p, widen, 0, unroll=2)

    def finish(k, _):
        v = turn[pl.ds(k, channels, stride=SUB), :]
        v = v - jnp.mean(v, axis=0, keepdims=True)
        v = v * lax.rsqrt(jnp.mean(v * v, axis=0, keepdims=True) + 1e-05) * gain
        res = (tn(v.astype(BF16), ow_ref[...]) * gate[k]).astype(BF16)
        out_ref[k] = res[:width]
        out_ref[k + rows] = res[width:]
        return 0

    lax.fori_loop(0, rows, finish, 0, unroll=UE)

    left(orecv.at[others, home], o_ss.at[0])

    @pl.when(at_mid)
    def _():
        left(orecv.at[others, moved], o_ss.at[0])
        left(orecv.at[:, moved], o_ss.at[1])


def fused(n_p, n_q, pair_array, lw, rw, lg, rg, gain, ow, og):
    channels = lw.shape[1]
    slab = channels // n_p * SUB
    rows = pair_array.shape[0] // 2
    dma = pltpu.SemaphoreType.DMA
    return pl.pallas_call(
        functools.partial(kernel, n_p, n_q),
        out_shape=pltpu.VMEM(pair_array.shape, BF16),
        in_specs=[pl.BlockSpec(memory_space=pltpu.HBM)] * 8,
        out_specs=pl.BlockSpec(memory_space=pltpu.VMEM),
        scratch_shapes=[
            pltpu.VMEM(pair_array.shape, BF16),
            *[pltpu.VMEM(lw.shape, BF16)] * 4,
            pltpu.VMEM((1, channels), F32),
            pltpu.VMEM(ow.shape, BF16),
            pltpu.VMEM(og.shape, BF16),
            dma((8,)),
            pltpu.VMEM((channels * SUB, LANES), F32),
            pltpu.VMEM((n_p, slab, LANES), BF16),
            pltpu.VMEM((n_p, slab, LANES), BF16),
            pltpu.VMEM((4, n_p, slab, LANES), BF16),
            pltpu.VMEM((2, n_p, slab, LANES), BF16),
            pltpu.VMEM((4, 2, 2, slab, LANES), BF16),
            pltpu.VMEM((n_p, slab, LANES), BF16),
            pltpu.VMEM((rows, LANES, channels), F32),
            dma((2,)),
            dma((2, len(CHUNKS) + 1)),
            dma((4,)),
            dma((6,)),
            dma((4, len(CHUNKS))),
            dma(()),
            dma((4, len(HOME))),
            dma((2,)),
            dma((2,)),
        ],
        compiler_params=pltpu.CompilerParams(
            collective_id=0, has_side_effects=True, vmem_limit_bytes=33_554_432
        ),
    )(*(
        pltpu.with_memory_space_constraint(a, pltpu.HBM)
        for a in (pair_array, lw, rw, lg, rg, gain.reshape(1, channels), ow, og)
    ))


def solution(mesh):
    n_p, n_q = mesh.shape["pr"], mesh.shape["pc"]

    def on_device(pair_array, lw, *rest):
        first, second, wide = pair_array.shape
        fits = (
            n_q == 4
            and first == 2 * SUB
            and second == 2 * first
            and n_p == 2 * n_q
            and 2 * second == LANES
            and wide == LANES
            and lw.shape[1] == LANES
            and n_p * sum(CHUNKS) == LANES
        )
        if fits:
            return fused(n_p, n_q, pair_array, lw, *rest)
        return plain(pair_array, lw, *rest)

    return jax.shard_map(
        on_device,
        mesh=mesh,
        in_specs=(P("pr", "pc", None), P(), P(), P(), P(), P(), P(), P()),
        out_specs=P("pr", "pc", None),
        check_vma=False,
    )
```

```python
import functools

import jax
import jax.numpy as jnp
from jax import lax
from jax.experimental import pallas as pl
from jax.experimental.pallas import tpu as pltpu
from jax.sharding import PartitionSpec as P

MESH = pl.DeviceIdType.MESH
BF16 = jnp.bfloat16
F32 = jnp.float32
LANES = 128
SUB = 16
STEP = 17
UF, UP, UE = 16, 8, 16


def unit_channels(values, channel_gain):
    centred = values - jnp.mean(values, axis=-1, keepdims=True)
    return (
        centred
        * lax.rsqrt(jnp.mean(centred * centred, axis=-1, keepdims=True) + 1e-05)
        * channel_gain
    )


def make_factors(pair_in, left_weight, right_weight, left_gate, right_gate):
    left = jnp.einsum("ijc,cd->ijd", pair_in, left_weight, preferred_element_type=F32)
    left = left * jax.nn.sigmoid(
        jnp.einsum("ijc,cd->ijd", pair_in, left_gate, preferred_element_type=F32)
    )
    right = jnp.einsum("ijc,cd->ijd", pair_in, right_weight, preferred_element_type=F32)
    right = right * jax.nn.sigmoid(
        jnp.einsum("ijc,cd->ijd", pair_in, right_gate, preferred_element_type=F32)
    )
    return (pair_in, left.astype(BF16), right.astype(BF16))


def to_pair(mixed, ready, mid_gain, out_weight, out_gate):
    scaled = unit_channels(mixed.astype(F32), mid_gain).astype(BF16)
    scaled = lax.optimization_barrier(scaled)
    gate = jax.nn.sigmoid(jnp.einsum("ijc,cd->ijd", ready, out_gate, preferred_element_type=F32))
    return (
        jnp.einsum("ijd,dc->ijc", scaled, out_weight, preferred_element_type=F32) * gate
    ).astype(BF16)


def plain(
    pair_array, left_weight, right_weight, left_gate, right_gate, mid_gain, out_weight, out_gate
):
    ready, left, right = make_factors(pair_array, left_weight, right_weight, left_gate, right_gate)
    count = pair_array.shape[0] * lax.axis_size("pr")
    left_lines, right_lines = (
        lax.all_to_all(left, "pr", split_axis=2, concat_axis=0, tiled=True),
        lax.all_to_all(right, "pr", split_axis=2, concat_axis=0, tiled=True),
    )
    strip = jnp.einsum(
        "kid,kjd->ijd",
        lax.all_gather(left_lines, "pc", axis=1, tiled=True),
        right_lines,
        preferred_element_type=F32,
    )
    strip = (strip * count ** (-0.5)).astype(BF16)
    mixed = lax.all_to_all(strip, "pr", split_axis=0, concat_axis=2, tiled=True)
    return to_pair(mixed, ready, mid_gain, out_weight, out_gate)


def nt(a, b):
    return lax.dot_general(a, b, (((1,), (1,)), ((), ())), preferred_element_type=F32)


def tn(a, b):
    return lax.dot_general(a, b, (((0,), (0,)), ((), ())), preferred_element_type=F32)


HOME = (3, 3)
MOVED = (4, 4, 2)
CHUNKS = HOME + MOVED
ORDER = ('M', 'N0', 'N1', 'O', 'T0', 'T1', 'g', 'F0', 'N2', 'C0', 'F1', 'N3', 'C1', 'N4', 'F2', 'D0', 'P0', 'Q0', 'P2', 'C2', 'G2', 'D1', 'P1', 'Q1', 'F3', 'P3', 'C3', 'G3', 'F4', 'P4', 'D2', 'Q2', 'C4', 'G4', 'D3', 'Q3', 'D4', 'Q4')
END_ORDER = ('L0', 'L1', 'B', 'L2', 'R2', 'L3', 'R3', 'L4', 'R4')
WHOLE = tuple(c for c in range(len(CHUNKS)) if f"G{c}" not in ORDER)


def kernel(
    n_p, n_q, x_hbm, lw_hbm, rw_hbm, lg_hbm, rg_hbm, gain_hbm, ow_hbm, og_hbm, out_ref,
    x_ref, w_ref, gain_ref, x_s, w_s, gain_s,
    turn, lsend, rsend, lbuf, rbuf, osend, orecv, gate,
    a_ss, a_rs, f_ss, own_rs, f_rs, e_ss, o_ss, o_rs,
):
    p = lax.axis_index("pr")
    q = lax.axis_index("pc")
    half = q // 2
    mid, end = 1 + half, 3 * half
    far_mid, far_end = 2 - half, 3 - 3 * half
    at_mid = q == mid
    per = lsend.shape[1] // SUB
    width = x_ref.shape[1]
    rows = x_ref.shape[0] // 2
    channels = n_p * per
    count = n_p * x_ref.shape[0]
    planes = (mid, end, far_mid, far_end)
    n_c = len(CHUNKS)
    part = [pl.ds(sum(CHUNKS[:c]) * SUB, CHUNKS[c] * SUB) for c in range(n_c)]
    others = pl.ds(1, n_p - 1)
    pair = pl.ds(0, 2)
    away = pl.ds(2, n_p - 2)
    n_h = len(HOME)
    home = pl.ds(0, sum(HOME) * SUB)
    moved = pl.ds(sum(HOME) * SUB, sum(MOVED) * SUB)

    bring_x = pltpu.make_async_copy(x_hbm, x_ref, x_s)
    bring_gain = pltpu.make_async_copy(gain_hbm, gain_ref, gain_s)
    bring_x.start()
    for at, src in enumerate((lw_hbm, lg_hbm, rw_hbm, rg_hbm, og_hbm, ow_hbm)):
        pltpu.make_async_copy(src, w_ref.at[at], w_s).start()
    bring_gain.start()

    barrier = pltpu.get_barrier_semaphore()
    def greet(to):
        pl.semaphore_signal(barrier, inc=1, device_id=to, device_id_type=MESH)

    for dp in range(1, n_p):
        greet((p ^ dp, q))

    @pl.when(at_mid)
    def _():
        greet((p, far_mid))
        greet((p, end))


    def pair_rows(k):
        return jnp.concatenate([x_ref[k], x_ref[k + rows]], axis=0)

    def factor(first, send):
        both = jnp.concatenate([w_ref[first].T, w_ref[first + 1].T], axis=0)

        def step(k, _):
            pr = nt(both, pair_rows(k))
            turn[pl.ds(k, channels, stride=STEP), :] = pr[:channels] * jax.nn.sigmoid(pr[channels:])
            return 0

        lax.fori_loop(0, rows, step, 0, unroll=UF)

        def cast(e, _):
            at = pl.multiple_of(e * per * STEP, per * STEP)
            for d in range(per):
                send[e, d * SUB : (d + 1) * SUB] = turn[pl.ds(at + d * STEP, SUB), :].astype(BF16)
            return 0

        lax.fori_loop(0, n_p, cast, 0, unroll=2)

    def remote(src, dst, send_sem, recv_sem, to):
        return pltpu.make_async_remote_copy(
            src_ref=src, dst_ref=dst, send_sem=send_sem, recv_sem=recv_sem,
            device_id=to, device_id_type=MESH,
        )

    def arrived(ref, sem):
        remote(ref, ref, sem, sem, (p, q)).wait_recv()

    def left(ref, sem):
        remote(ref, ref, sem, sem, (p, q)).wait_send()

    def spread(kind, send, buf, order):
        def give(dp, lines, at):
            remote(
                send.at[p ^ dp, lines], buf.at[0, dp, lines],
                a_ss, a_rs.at[kind, at], (p ^ dp, q),
            ).start()

        give(1, slice(None), n_c)
        for c in order:
            for dp in range(n_p - 1, 1, -1):
                give(dp, part[c], c)

    def own(buf, slot_from, slot_to, at, to, slots, lines=slice(None)):
        remote(
            buf.at[slot_from, slots, lines], buf.at[slot_to, slots, lines],
            f_ss.at[at % 2], own_rs.at[at], to,
        ).start()

    def pass_on(buf, slot_from, slot_to, at, c, to):
        remote(
            buf.at[slot_from, away, part[c]], buf.at[slot_to, away, part[c]],
            f_ss.at[at % 2], f_rs.at[at, c], to,
        ).start()

    def to_end(slot_from, slot_to, c):
        remote(
            lbuf.at[slot_from, :, part[c]], lbuf.at[slot_to, :, part[c]],
            e_ss, f_rs.at[slot_to, c], (p, end),
        ).start()

    pltpu.make_async_copy(w_ref, w_ref, w_s).wait()
    bring_gain.wait()
    bring_x.wait()
    factor(0, lsend)
    pl.semaphore_wait(barrier, n_p)
    spread(0, lsend, lbuf, range(n_c))
    lbuf[0, 0] = lsend[p]

    @pl.when(at_mid)
    def _():
        own(lbuf, 0, 2, 2, (p, far_mid), 0)

    @pl.when(jnp.logical_not(at_mid))
    def _():
        own(lbuf, 0, 1, 0, (p, mid), 0)

    factor(2, rsend)
    rbuf[0, 0] = rsend[p]
    spread(1, rsend, rbuf, (*range(n_h, n_c), *range(n_h)))

    def make_gate(k, _):
        gate[k] = jax.nn.sigmoid(
            jnp.dot(pair_rows(k), w_ref[4], preferred_element_type=F32)
        )
        return 0

    def gates():
        lax.fori_loop(0, rows, make_gate, 0, unroll=4)

    low = lax.broadcasted_iota(jnp.int32, (SUB, LANES), 1) < width

    def multiply(g, c, plane, sides):
        def products(d, _):
            at = pl.ds(pl.multiple_of(d * SUB, SUB), SUB)
            lines = lbuf[g, :, at, :].reshape(n_p * SUB, LANES)
            right = [rbuf[j, :, at, :].reshape(n_p * SUB, LANES) for j in range(sides)]
            sums = tn(lines, right[0] if sides == 1 else jnp.concatenate(right, axis=1))
            for j in range(sides):
                acc = sums[:, j * LANES : (j + 1) * LANES]
                for b in range(2):
                    top = b * 2 * SUB
                    a0, c0 = acc[top : top + SUB], acc[top + SUB : top + 2 * SUB]
                    b0 = acc[width + top : width + top + SUB]
                    d0 = acc[width + top + SUB : width + top + 2 * SUB]
                    tile = jnp.where(low, a0, d0) + pltpu.roll(
                        jnp.where(low, c0, b0), width, 1
                    )
                    osend[g, b, j, at, :] = (tile * count ** (-0.5)).astype(BF16)
            return 0

        first = sum(CHUNKS[:c])
        lax.fori_loop(first, first + CHUNKS[c], products, 0, unroll=CHUNKS[c])
        done = o_rs.at[0 if c < n_h else 1]
        for b in range(2):
            to_p = plane * 2 + b
            if sides == 2:
                remote(
                    osend.at[g, b, 1, part[c]], orecv.at[p, part[c]],
                    o_ss.at[1], done, (to_p, end),
                ).start()

            @pl.when(to_p != p)
            def _():
                remote(
                    osend.at[g, b, 0, part[c]], orecv.at[p, part[c]],
                    o_ss.at[0], done, (to_p, q),
                ).start()

            @pl.when(to_p == p)
            def _():
                orecv[p, part[c]] = osend[g, b, 0, part[c]]

    turn_of = p // 2

    def rotated(n, c, plane_of, sides):
        for t in range(n):
            g = lax.rem(turn_of + t, n)
            plane = plane_of[n - 1]
            for at in range(n - 1):
                plane = jnp.where(g == at, plane_of[at], plane)
            multiply(g, c, plane, sides)

    @pl.when(jnp.logical_not(at_mid))
    def _():
        def pass_left(c):
            arrived(lbuf.at[0, away, part[c]], a_rs.at[0, c])
            pass_on(lbuf, 0, 1, 0, c, (p, mid))

        def pass_right(c):
            arrived(rbuf.at[0, away, part[c]], a_rs.at[1, c])
            pass_on(rbuf, 0, 1, 1, c, (p, mid))

        arrived(lbuf.at[0, 1], a_rs.at[0, n_c])
        own(lbuf, 0, 1, 0, (p, mid), 1)

        def right_pair():
            arrived(rbuf.at[0, 1], a_rs.at[1, n_c])
            own(rbuf, 0, 1, 1, (p, mid), pair, moved)

        for step in END_ORDER:
            if step == "B":
                right_pair()
            else:
                {"L": pass_left, "R": pass_right}[step[0]](int(step[1:]))
        gates()
        for c in range(n_h):
            arrived(rbuf.at[0, away, part[c]], a_rs.at[1, c])
            arrived(lbuf.at[1, :, part[c]], f_rs.at[1, c])
            arrived(lbuf.at[2, :, part[c]], f_rs.at[2, c])
            rotated(3, c, (end, mid, far_mid), 1)
        for c in range(n_h):
            arrived(lbuf.at[3, :, part[c]], f_rs.at[3, c])
            multiply(3, c, far_end, 1)
        left(lbuf.at[0], f_ss.at[0])
        left(lbuf.at[0, :, moved], f_ss.at[1])

    @pl.when(at_mid)
    def _():
        def pass_near(c):
            arrived(lbuf.at[0, away, part[c]], a_rs.at[0, c])
            pass_on(lbuf, 0, 2, 2, c, (p, far_mid))

        def pass_far(c):
            arrived(lbuf.at[1, away, part[c]], f_rs.at[0, c])
            pass_on(lbuf, 1, 3, 3, c, (p, far_mid))

        def came(c):
            if c == 0:
                arrived(lbuf.at[2, pair], own_rs.at[2])
            arrived(lbuf.at[2, away, part[c]], f_rs.at[2, c])
            if c < n_h:
                to_end(2, 2, c)

        def near(c):
            if c == n_h:
                arrived(rbuf.at[1, pair, moved], own_rs.at[1])
            arrived(rbuf.at[0, away, part[c]], a_rs.at[1, c])
            if c >= n_h:
                arrived(rbuf.at[1, away, part[c]], f_rs.at[1, c])
            rotated(3 if c in WHOLE else 2, c, planes, 1 if c < n_h else 2)

        def near_to_end(c):
            to_end(0, 1, c)

        def far_near(c):
            multiply(2, c, far_mid, 1 if c < n_h else 2)

        def mate():
            arrived(lbuf.at[0, 1], a_rs.at[0, n_c])
            own(lbuf, 0, 2, 2, (p, far_mid), 1)

        def onward():
            arrived(lbuf.at[1, pair], own_rs.at[0])
            own(lbuf, 1, 3, 3, (p, far_mid), pair)

        def came_far(c):
            if c == 0:
                arrived(lbuf.at[3, pair], own_rs.at[3])
            arrived(lbuf.at[3, away, part[c]], f_rs.at[3, c])
            if c < n_h:
                to_end(3, 3, c)

        def last(c):
            multiply(3, c, far_end, 1 if c < n_h else 2)

        first_right = next(step for step in ORDER if step[0] == "P")
        act = {"N": pass_near, "F": pass_far, "C": came, "P": near, "G": far_near, "T": near_to_end, "D": came_far, "Q": last}
        alone = {"M": mate, "O": onward, "g": gates}
        for step in ORDER:
            if step == first_right:
                arrived(rbuf.at[0, 1], a_rs.at[1, n_c])
            if step in alone:
                alone[step]()
            else:
                act[step[0]](int(step[1:]))
        left(lbuf.at[0], f_ss.at[0])
        left(lbuf.at[0], f_ss.at[1])
        left(lbuf.at[pl.ds(1, 3), :, home], e_ss)

    gain = jnp.broadcast_to(gain_ref[...], (channels, channels)).T
    left(lbuf.at[pl.ds(0, 2), others], a_ss)

    arrived(orecv.at[others, home], o_rs.at[0])

    @pl.when(at_mid)
    def _():
        arrived(orecv.at[others, moved], o_rs.at[1])

    @pl.when(jnp.logical_not(at_mid))
    def _():
        arrived(orecv.at[:, moved], o_rs.at[1])

    def widen(e, _):
        at = pl.multiple_of(e * per * STEP, per * STEP)
        for d in range(per):
            turn[pl.ds(at + d * STEP, SUB), :] = orecv[e, d * SUB : (d + 1) * SUB].astype(F32)
        return 0

    lax.fori_loop(0, n_p, widen, 0, unroll=2)

    def finish(k, _):
        v = turn[pl.ds(k, channels, stride=STEP), :]
        v = v - jnp.mean(v, axis=0, keepdims=True)
        v = v * lax.rsqrt(jnp.mean(v * v, axis=0, keepdims=True) + 1e-05) * gain
        res = (tn(v.astype(BF16), w_ref[5]) * gate[k]).astype(BF16)
        out_ref[k] = res[:width]
        out_ref[k + rows] = res[width:]
        return 0

    lax.fori_loop(0, rows, finish, 0, unroll=UE)

    left(orecv.at[others, home], o_ss.at[0])

    @pl.when(at_mid)
    def _():
        left(orecv.at[others, moved], o_ss.at[0])
        left(orecv.at[:, moved], o_ss.at[1])


def fused(n_p, n_q, pair_array, lw, rw, lg, rg, gain, ow, og):
    channels = lw.shape[1]
    slab = channels // n_p * SUB
    rows = pair_array.shape[0] // 2
    dma = pltpu.SemaphoreType.DMA
    return pl.pallas_call(
        functools.partial(kernel, n_p, n_q),
        out_shape=pltpu.VMEM(pair_array.shape, BF16),
        in_specs=[pl.BlockSpec(memory_space=pltpu.HBM)] * 8,
        out_specs=pl.BlockSpec(memory_space=pltpu.VMEM),
        scratch_shapes=[
            pltpu.VMEM(pair_array.shape, BF16),
            pltpu.VMEM((6, *lw.shape), BF16),
            pltpu.VMEM((1, channels), F32),
            dma(()),
            dma(()),
            dma(()),
            pltpu.VMEM((channels * STEP, LANES), F32),
            pltpu.VMEM((n_p, slab, LANES), BF16),
            pltpu.VMEM((n_p, slab, LANES), BF16),
            pltpu.VMEM((4, n_p, slab, LANES), BF16),
            pltpu.VMEM((2, n_p, slab, LANES), BF16),
            pltpu.VMEM((4, 2, 2, slab, LANES), BF16),
            pltpu.VMEM((n_p, slab, LANES), BF16),
            pltpu.VMEM((rows, LANES, channels), F32),
            dma(()),
            dma((2, len(CHUNKS) + 1)),
            dma((2,)),
            dma((4,)),
            dma((4, len(CHUNKS))),
            dma(()),
            dma((2,)),
            dma((2,)),
        ],
        compiler_params=pltpu.CompilerParams(
            collective_id=0, has_side_effects=True, vmem_limit_bytes=33_554_432
        ),
    )(*(
        pltpu.with_memory_space_constraint(a, pltpu.HBM)
        for a in (pair_array, lw, rw, lg, rg, gain.reshape(1, channels), ow, og)
    ))


def solution(mesh):
    n_p, n_q = mesh.shape["pr"], mesh.shape["pc"]

    def on_device(pair_array, lw, *rest):
        first, second, wide = pair_array.shape
        fits = (
            n_q == 4
            and first == 2 * SUB
            and second == 2 * first
            and n_p == 2 * n_q
            and 2 * second == LANES
            and wide == LANES
            and lw.shape[1] == LANES
            and n_p * sum(CHUNKS) == LANES
        )
        if fits:
            return fused(n_p, n_q, pair_array, lw, *rest)
        return plain(pair_array, lw, *rest)

    return jax.shard_map(
        on_device,
        mesh=mesh,
        in_specs=(P("pr", "pc", None), P(), P(), P(), P(), P(), P(), P()),
        out_specs=P("pr", "pc", None),
        check_vma=False,
    )
```

```python
import functools

import jax
import jax.numpy as jnp
from jax import lax
from jax.experimental import pallas as pl
from jax.experimental.pallas import tpu as pltpu
from jax.sharding import PartitionSpec as P

MESH = pl.DeviceIdType.MESH
BF16 = jnp.bfloat16
F32 = jnp.float32
LANES = 128
SUB = 16
STEP = 17
UF, UP, UE = 16, 8, 16


def unit_channels(values, channel_gain):
    centred = values - jnp.mean(values, axis=-1, keepdims=True)
    return (
        centred
        * lax.rsqrt(jnp.mean(centred * centred, axis=-1, keepdims=True) + 1e-05)
        * channel_gain
    )


def make_factors(pair_in, left_weight, right_weight, left_gate, right_gate):
    left = jnp.einsum("ijc,cd->ijd", pair_in, left_weight, preferred_element_type=F32)
    left = left * jax.nn.sigmoid(
        jnp.einsum("ijc,cd->ijd", pair_in, left_gate, preferred_element_type=F32)
    )
    right = jnp.einsum("ijc,cd->ijd", pair_in, right_weight, preferred_element_type=F32)
    right = right * jax.nn.sigmoid(
        jnp.einsum("ijc,cd->ijd", pair_in, right_gate, preferred_element_type=F32)
    )
    return (pair_in, left.astype(BF16), right.astype(BF16))


def to_pair(mixed, ready, mid_gain, out_weight, out_gate):
    scaled = unit_channels(mixed.astype(F32), mid_gain).astype(BF16)
    scaled = lax.optimization_barrier(scaled)
    gate = jax.nn.sigmoid(jnp.einsum("ijc,cd->ijd", ready, out_gate, preferred_element_type=F32))
    return (
        jnp.einsum("ijd,dc->ijc", scaled, out_weight, preferred_element_type=F32) * gate
    ).astype(BF16)


def plain(
    pair_array, left_weight, right_weight, left_gate, right_gate, mid_gain, out_weight, out_gate
):
    ready, left, right = make_factors(pair_array, left_weight, right_weight, left_gate, right_gate)
    count = pair_array.shape[0] * lax.axis_size("pr")
    left_lines, right_lines = (
        lax.all_to_all(left, "pr", split_axis=2, concat_axis=0, tiled=True),
        lax.all_to_all(right, "pr", split_axis=2, concat_axis=0, tiled=True),
    )
    strip = jnp.einsum(
        "kid,kjd->ijd",
        lax.all_gather(left_lines, "pc", axis=1, tiled=True),
        right_lines,
        preferred_element_type=F32,
    )
    strip = (strip * count ** (-0.5)).astype(BF16)
    mixed = lax.all_to_all(strip, "pr", split_axis=0, concat_axis=2, tiled=True)
    return to_pair(mixed, ready, mid_gain, out_weight, out_gate)


def nt(a, b):
    return lax.dot_general(a, b, (((1,), (1,)), ((), ())), preferred_element_type=F32)


def tn(a, b):
    return lax.dot_general(a, b, (((0,), (0,)), ((), ())), preferred_element_type=F32)


HOME = (3, 3)
MOVED = (4, 3)
EDGE = (2, 4)
CHUNKS = tuple(HOME + MOVED + (edge,) for edge in EDGE)
COUNT = tuple(sum(sizes) for sizes in CHUNKS)
ORDER = ('M', 'N0', 'N1', 'O', 'T0', 'T1', 'g', 'F0', 'N2', 'C0', 'F1', 'N3', 'C1', 'N4', 'F2', 'D0', 'P0', 'Q0', 'P2', 'C2', 'G2', 'D1', 'P1', 'Q1', 'F3', 'P3', 'C3', 'G3', 'F4', 'P4', 'D2', 'Q2', 'C4', 'G4', 'D3', 'Q3', 'D4', 'Q4')
END_ORDER = ('L0', 'L1', 'B', 'L2', 'R2', 'L3', 'R3', 'L4', 'R4')
WHOLE = tuple(c for c in range(len(CHUNKS[0])) if f"G{c}" not in ORDER)


def kernel(
    n_p, n_q, x_hbm, lw_hbm, rw_hbm, lg_hbm, rg_hbm, gain_hbm, ow_hbm, og_hbm, out_ref,
    x_ref, w_ref, gain_ref, x_s, w_s, gain_s,
    turn, lsend, rsend, lbuf, rbuf, osend, orecv, gate,
    a_ss, a_rs, b_rs, f_ss, own_rs, f_rs, e_ss, o_ss, o_rs,
):
    p = lax.axis_index("pr")
    q = lax.axis_index("pc")
    half = q // 2
    mid, end = 1 + half, 3 * half
    far_mid, far_end = 2 - half, 3 - 3 * half
    at_mid = q == mid
    width = x_ref.shape[1]
    rows = x_ref.shape[0] // 2
    channels = w_ref.shape[2]
    count = n_p * x_ref.shape[0]
    planes = (mid, end, far_mid, far_end)
    n_c = len(CHUNKS[0])
    n_h = len(HOME)
    n_home = sum(HOME)
    parts = [
        [pl.ds(sum(sizes[:c]) * SUB, sizes[c] * SUB) for c in range(n_c)] for sizes in CHUNKS
    ]
    wholes = [pl.ds(0, n * SUB) for n in COUNT]
    moveds = [pl.ds(n_home * SUB, (n - n_home) * SUB) for n in COUNT]
    home = pl.ds(0, n_home * SUB)
    others = pl.ds(1, n_p - 1)
    pair = pl.ds(0, 2)
    away = pl.ds(2, n_p - 2)
    core = lax.rem(p, 2)

    def by_core(act):
        for k in range(2):

            @pl.when(core == k)
            def _():
                act(k)

    bring_x = pltpu.make_async_copy(x_hbm, x_ref, x_s)
    bring_gain = pltpu.make_async_copy(gain_hbm, gain_ref, gain_s)
    bring_x.start()
    for at, src in enumerate((lw_hbm, lg_hbm, rw_hbm, rg_hbm, og_hbm, ow_hbm)):
        pltpu.make_async_copy(src, w_ref.at[at], w_s).start()
    bring_gain.start()

    barrier = pltpu.get_barrier_semaphore()
    def greet(to):
        pl.semaphore_signal(barrier, inc=1, device_id=to, device_id_type=MESH)

    for dp in range(1, n_p):
        greet((p ^ dp, q))

    @pl.when(at_mid)
    def _():
        greet((p, far_mid))
        greet((p, end))


    def pair_rows(k):
        return jnp.concatenate([x_ref[k], x_ref[k + rows]], axis=0)

    def factor(first, send):
        both = jnp.concatenate([w_ref[first].T, w_ref[first + 1].T], axis=0)

        def step(k, _):
            pr = nt(both, pair_rows(k))
            turn[pl.ds(k, channels, stride=STEP), :] = pr[:channels] * jax.nn.sigmoid(pr[channels:])
            return 0

        lax.fori_loop(0, rows, step, 0, unroll=UF)

        def cast(e, _):
            for k in range(2):
                for d in range(COUNT[k]):
                    at = (e * sum(COUNT) + k * COUNT[0] + d) * STEP
                    send[e * 2 + k, d * SUB : (d + 1) * SUB] = turn[pl.ds(at, SUB), :].astype(BF16)
            return 0

        lax.fori_loop(0, n_p // 2, cast, 0)

    def remote(src, dst, send_sem, recv_sem, to):
        return pltpu.make_async_remote_copy(
            src_ref=src, dst_ref=dst, send_sem=send_sem, recv_sem=recv_sem,
            device_id=to, device_id_type=MESH,
        )

    def arrived(ref, sem):
        remote(ref, ref, sem, sem, (p, q)).wait_recv()

    def left(ref, sem):
        remote(ref, ref, sem, sem, (p, q)).wait_send()

    def spread(k, sems, send, buf, pieces):
        def give(dp, lines, sem):
            remote(
                send.at[p ^ dp, lines], buf.at[0, dp, lines],
                a_ss.at[dp & 1], sem, (p ^ dp, q),
            ).start()

        n = len(pieces[0])
        give(1, wholes[1 - k], sems.at[n])
        for at in range(n):
            for dp in range(n_p - 1, 1, -1):
                give(dp, pieces[k ^ (dp & 1)][at], sems.at[at])

    def own(buf, slot_from, slot_to, at, to, slots, lines):
        remote(
            buf.at[slot_from, slots, lines], buf.at[slot_to, slots, lines],
            f_ss.at[at % 2], own_rs.at[at], to,
        ).start()

    def to_end(slot_from, slot_to, c):
        remote(
            lbuf.at[slot_from, :, parts[0][c]], lbuf.at[slot_to, :, parts[0][c]],
            e_ss, f_rs.at[slot_to, c], (p, end),
        ).start()

    pltpu.make_async_copy(w_ref, w_ref, w_s).wait()
    bring_gain.wait()
    bring_x.wait()
    factor(0, lsend)
    pl.semaphore_wait(barrier, n_p)

    def send_left(k):
        lines = wholes[k]
        lbuf[0, 0, lines] = lsend[p, lines]

        @pl.when(at_mid)
        def _():
            own(lbuf, 0, 2, 2, (p, far_mid), 0, lines)

        @pl.when(jnp.logical_not(at_mid))
        def _():
            own(lbuf, 0, 1, 0, (p, mid), 0, lines)

        spread(k, a_rs, lsend, lbuf, parts)

    by_core(send_left)
    factor(2, rsend)

    def make_gate(k, _):
        gate[k] = jax.nn.sigmoid(
            jnp.dot(pair_rows(k), w_ref[4], preferred_element_type=F32)
        )
        return 0

    def gates():
        lax.fori_loop(0, rows, make_gate, 0, unroll=4)

    low = lax.broadcasted_iota(jnp.int32, (SUB, LANES), 1) < width

    def pass_on_core(k):
        sizes, part, whole, moved = CHUNKS[k], parts[k], wholes[k], moveds[k]

        rbuf[0, 0, whole] = rsend[p, whole]
        spread(k, b_rs, rsend, rbuf, [(*parts[n][n_h:], home) for n in range(2)])

        def pass_on(buf, slot_from, slot_to, at, c, to):
            remote(
                buf.at[slot_from, away, part[c]], buf.at[slot_to, away, part[c]],
                f_ss.at[at % 2], f_rs.at[at, c], to,
            ).start()

        def multiply(g, c, plane, sides):
            first = sum(sizes[:c])
            done = o_rs.at[0 if c < n_h else 1 + k]

            def some(these):
                def products(d, _):
                    at = pl.ds(pl.multiple_of(d * SUB, SUB), SUB)
                    lines = lbuf[g, :, at, :].reshape(n_p * SUB, LANES)
                    right = [rbuf[j, :, at, :].reshape(n_p * SUB, LANES) for j in these]
                    sums = tn(lines, right[0] if len(these) == 1 else jnp.concatenate(right, axis=1))
                    for n, j in enumerate(these):
                        acc = sums[:, n * LANES : (n + 1) * LANES]
                        for b in range(2):
                            top = b * 2 * SUB
                            a0, c0 = acc[top : top + SUB], acc[top + SUB : top + 2 * SUB]
                            b0 = acc[width + top : width + top + SUB]
                            d0 = acc[width + top + SUB : width + top + 2 * SUB]
                            tile = jnp.where(low, a0, d0) + pltpu.roll(
                                jnp.where(low, c0, b0), width, 1
                            )
                            osend[g, b, j, at, :] = (tile * count ** (-0.5)).astype(BF16)
                    return 0

                lax.fori_loop(first, first + sizes[c], products, 0, unroll=sizes[c])

            def give_end():
                for b in range(2):
                    remote(
                        osend.at[g, b, 1, part[c]], orecv.at[p, part[c]],
                        o_ss.at[1], done, (plane * 2 + b, end),
                    ).start()

            if sides == 2 and c == n_c - 1:
                some((1,))
                give_end()
                some((0,))
            else:
                some(tuple(range(sides)))
                if sides == 2:
                    give_end()
            for b in range(2):
                to_p = plane * 2 + b

                @pl.when(to_p != p)
                def _():
                    remote(
                        osend.at[g, b, 0, part[c]], orecv.at[p, part[c]],
                        o_ss.at[0], done, (to_p, q),
                    ).start()

                @pl.when(to_p == p)
                def _():
                    orecv[p, part[c]] = osend[g, b, 0, part[c]]

        turn_of = p // 2

        def rotated(n, c, plane_of, sides):
            for t in range(n):
                g = lax.rem(turn_of + t, n)
                plane = plane_of[n - 1]
                for at in range(n - 1):
                    plane = jnp.where(g == at, plane_of[at], plane)
                multiply(g, c, plane, sides)

        @pl.when(jnp.logical_not(at_mid))
        def _():
            def pass_left(c):
                arrived(lbuf.at[0, away, part[c]], a_rs.at[c])
                pass_on(lbuf, 0, 1, 0, c, (p, mid))

            def pass_right(c):
                arrived(rbuf.at[0, away, part[c]], b_rs.at[c - n_h])
                pass_on(rbuf, 0, 1, 1, c, (p, mid))

            arrived(lbuf.at[0, 1, whole], a_rs.at[n_c])
            own(lbuf, 0, 1, 0, (p, mid), 1, whole)

            def right_pair():
                arrived(rbuf.at[0, 1, whole], b_rs.at[n_c - n_h + 1])
                own(rbuf, 0, 1, 1, (p, mid), pair, moved)

            for step in END_ORDER:
                if step == "B":
                    right_pair()
                else:
                    {"L": pass_left, "R": pass_right}[step[0]](int(step[1:]))
            gates()
            for c in range(n_h):
                if c == 0:
                    arrived(rbuf.at[0, away, home], b_rs.at[n_c - n_h])
                arrived(lbuf.at[1, :, part[c]], f_rs.at[1, c])
                arrived(lbuf.at[2, :, part[c]], f_rs.at[2, c])
                rotated(3, c, (end, mid, far_mid), 1)
            for c in range(n_h):
                arrived(lbuf.at[3, :, part[c]], f_rs.at[3, c])
                multiply(3, c, far_end, 1)
            left(lbuf.at[0, :, whole], f_ss.at[0])
            left(lbuf.at[0, :, moved], f_ss.at[1])

        @pl.when(at_mid)
        def _():
            def pass_near(c):
                arrived(lbuf.at[0, away, part[c]], a_rs.at[c])
                pass_on(lbuf, 0, 2, 2, c, (p, far_mid))

            def pass_far(c):
                arrived(lbuf.at[1, away, part[c]], f_rs.at[0, c])
                pass_on(lbuf, 1, 3, 3, c, (p, far_mid))

            def came(c):
                if c == 0:
                    arrived(lbuf.at[2, pair, whole], own_rs.at[2])
                arrived(lbuf.at[2, away, part[c]], f_rs.at[2, c])
                if c < n_h:
                    to_end(2, 2, c)

            def near(c):
                if c == n_h:
                    arrived(rbuf.at[1, pair, moved], own_rs.at[1])
                if c == 0:
                    arrived(rbuf.at[0, away, home], b_rs.at[n_c - n_h])
                if c >= n_h:
                    arrived(rbuf.at[0, away, part[c]], b_rs.at[c - n_h])
                    arrived(rbuf.at[1, away, part[c]], f_rs.at[1, c])
                rotated(3 if c in WHOLE else 2, c, planes, 1 if c < n_h else 2)

            def near_to_end(c):
                to_end(0, 1, c)

            def far_near(c):
                multiply(2, c, far_mid, 1 if c < n_h else 2)

            def mate():
                arrived(lbuf.at[0, 1, whole], a_rs.at[n_c])
                own(lbuf, 0, 2, 2, (p, far_mid), 1, whole)

            def onward():
                arrived(lbuf.at[1, pair, whole], own_rs.at[0])
                own(lbuf, 1, 3, 3, (p, far_mid), pair, whole)

            def came_far(c):
                if c == 0:
                    arrived(lbuf.at[3, pair, whole], own_rs.at[3])
                arrived(lbuf.at[3, away, part[c]], f_rs.at[3, c])
                if c < n_h:
                    to_end(3, 3, c)

            def last(c):
                multiply(3, c, far_end, 1 if c < n_h else 2)

            first_right = next(step for step in ORDER if step[0] == "P")
            act = {"N": pass_near, "F": pass_far, "C": came, "P": near, "G": far_near, "T": near_to_end, "D": came_far, "Q": last}
            alone = {"M": mate, "O": onward, "g": gates}
            for step in ORDER:
                if step == first_right:
                    arrived(rbuf.at[0, 1, whole], b_rs.at[n_c - n_h + 1])
                if step in alone:
                    alone[step]()
                else:
                    act[step[0]](int(step[1:]))
            left(lbuf.at[0, :, whole], f_ss.at[0])
            left(lbuf.at[0, :, whole], f_ss.at[1])
            left(lbuf.at[pl.ds(1, 3), :, home], e_ss)

    by_core(pass_on_core)
    gain = jnp.broadcast_to(gain_ref[...], (channels, channels)).T

    def close(k):
        left(lbuf.at[pl.ds(0, 2), pl.ds(0, n_p // 2 - 1), wholes[k]], a_ss.at[0])
        left(lbuf.at[pl.ds(0, 2), pl.ds(0, n_p // 2), wholes[1 - k]], a_ss.at[1])
        arrived(orecv.at[others, home], o_rs.at[0])
        arrived(orecv.at[pl.ds(0, n_p // 2), moveds[1 - k]], o_rs.at[2 - k])

        @pl.when(at_mid)
        def _():
            arrived(orecv.at[pl.ds(0, n_p // 2 - 1), moveds[k]], o_rs.at[1 + k])

        @pl.when(jnp.logical_not(at_mid))
        def _():
            arrived(orecv.at[pl.ds(0, n_p // 2), moveds[k]], o_rs.at[1 + k])

    by_core(close)

    def widen(e, _):
        for k in range(2):
            for d in range(COUNT[k]):
                at = (e * sum(COUNT) + k * COUNT[0] + d) * STEP
                turn[pl.ds(at, SUB), :] = orecv[e * 2 + k, d * SUB : (d + 1) * SUB].astype(F32)
        return 0

    lax.fori_loop(0, n_p // 2, widen, 0)

    def finish(k, _):
        v = turn[pl.ds(k, channels, stride=STEP), :]
        v = v - jnp.mean(v, axis=0, keepdims=True)
        v = v * lax.rsqrt(jnp.mean(v * v, axis=0, keepdims=True) + 1e-05) * gain
        res = (tn(v.astype(BF16), w_ref[5]) * gate[k]).astype(BF16)
        out_ref[k] = res[:width]
        out_ref[k + rows] = res[width:]
        return 0

    lax.fori_loop(0, rows, finish, 0, unroll=UE)

    left(orecv.at[others, home], o_ss.at[0])

    def leave(k):
        left(orecv.at[others, moveds[k]], o_ss.at[0])
        left(orecv.at[:, moveds[k]], o_ss.at[1])

    @pl.when(at_mid)
    def _():
        by_core(leave)


def fused(n_p, n_q, pair_array, lw, rw, lg, rg, gain, ow, og):
    channels = lw.shape[1]
    slab = max(COUNT) * SUB
    rows = pair_array.shape[0] // 2
    dma = pltpu.SemaphoreType.DMA
    return pl.pallas_call(
        functools.partial(kernel, n_p, n_q),
        out_shape=pltpu.VMEM(pair_array.shape, BF16),
        in_specs=[pl.BlockSpec(memory_space=pltpu.HBM)] * 8,
        out_specs=pl.BlockSpec(memory_space=pltpu.VMEM),
        scratch_shapes=[
            pltpu.VMEM(pair_array.shape, BF16),
            pltpu.VMEM((6, *lw.shape), BF16),
            pltpu.VMEM((1, channels), F32),
            dma(()),
            dma(()),
            dma(()),
            pltpu.VMEM((channels * STEP, LANES), F32),
            pltpu.VMEM((n_p, slab, LANES), BF16),
            pltpu.VMEM((n_p, slab, LANES), BF16),
            pltpu.VMEM((4, n_p, slab, LANES), BF16),
            pltpu.VMEM((2, n_p, slab, LANES), BF16),
            pltpu.VMEM((4, 2, 2, slab, LANES), BF16),
            pltpu.VMEM((n_p, slab, LANES), BF16),
            pltpu.VMEM((rows, LANES, channels), F32),
            dma((2,)),
            dma((len(CHUNKS[0]) + 1,)),
            dma((len(MOVED) + 3,)),
            dma((2,)),
            dma((4,)),
            dma((4, len(CHUNKS[0]))),
            dma(()),
            dma((2,)),
            dma((3,)),
        ],
        compiler_params=pltpu.CompilerParams(
            collective_id=0, has_side_effects=True, vmem_limit_bytes=33_554_432
        ),
    )(*(
        pltpu.with_memory_space_constraint(a, pltpu.HBM)
        for a in (pair_array, lw, rw, lg, rg, gain.reshape(1, channels), ow, og)
    ))


def solution(mesh):
    n_p, n_q = mesh.shape["pr"], mesh.shape["pc"]

    def on_device(pair_array, lw, *rest):
        first, second, wide = pair_array.shape
        fits = (
            n_q == 4
            and first == 2 * SUB
            and second == 2 * first
            and n_p == 2 * n_q
            and 2 * second == LANES
            and wide == LANES
            and lw.shape[1] == LANES
            and n_p // 2 * sum(COUNT) == LANES
        )
        if fits:
            return fused(n_p, n_q, pair_array, lw, *rest)
        return plain(pair_array, lw, *rest)

    return jax.shard_map(
        on_device,
        mesh=mesh,
        in_specs=(P("pr", "pc", None), P(), P(), P(), P(), P(), P(), P()),
        out_specs=P("pr", "pc", None),
        check_vma=False,
    )
```

```python
import functools

import jax
import jax.numpy as jnp
from jax import lax
from jax.experimental import pallas as pl
from jax.experimental.pallas import tpu as pltpu
from jax.sharding import PartitionSpec as P

MESH = pl.DeviceIdType.MESH
BF16 = jnp.bfloat16
F32 = jnp.float32
LANES = 128
SUB = 16
STEP = 17
UF, UP, UE = 16, 8, 16


def unit_channels(values, channel_gain):
    centred = values - jnp.mean(values, axis=-1, keepdims=True)
    return (
        centred
        * lax.rsqrt(jnp.mean(centred * centred, axis=-1, keepdims=True) + 1e-05)
        * channel_gain
    )


def make_factors(pair_in, left_weight, right_weight, left_gate, right_gate):
    left = jnp.einsum("ijc,cd->ijd", pair_in, left_weight, preferred_element_type=F32)
    left = left * jax.nn.sigmoid(
        jnp.einsum("ijc,cd->ijd", pair_in, left_gate, preferred_element_type=F32)
    )
    right = jnp.einsum("ijc,cd->ijd", pair_in, right_weight, preferred_element_type=F32)
    right = right * jax.nn.sigmoid(
        jnp.einsum("ijc,cd->ijd", pair_in, right_gate, preferred_element_type=F32)
    )
    return (pair_in, left.astype(BF16), right.astype(BF16))


def to_pair(mixed, ready, mid_gain, out_weight, out_gate):
    scaled = unit_channels(mixed.astype(F32), mid_gain).astype(BF16)
    scaled = lax.optimization_barrier(scaled)
    gate = jax.nn.sigmoid(jnp.einsum("ijc,cd->ijd", ready, out_gate, preferred_element_type=F32))
    return (
        jnp.einsum("ijd,dc->ijc", scaled, out_weight, preferred_element_type=F32) * gate
    ).astype(BF16)


def plain(
    pair_array, left_weight, right_weight, left_gate, right_gate, mid_gain, out_weight, out_gate
):
    ready, left, right = make_factors(pair_array, left_weight, right_weight, left_gate, right_gate)
    count = pair_array.shape[0] * lax.axis_size("pr")
    left_lines, right_lines = (
        lax.all_to_all(left, "pr", split_axis=2, concat_axis=0, tiled=True),
        lax.all_to_all(right, "pr", split_axis=2, concat_axis=0, tiled=True),
    )
    strip = jnp.einsum(
        "kid,kjd->ijd",
        lax.all_gather(left_lines, "pc", axis=1, tiled=True),
        right_lines,
        preferred_element_type=F32,
    )
    strip = (strip * count ** (-0.5)).astype(BF16)
    mixed = lax.all_to_all(strip, "pr", split_axis=0, concat_axis=2, tiled=True)
    return to_pair(mixed, ready, mid_gain, out_weight, out_gate)


def nt(a, b):
    return lax.dot_general(a, b, (((1,), (1,)), ((), ())), preferred_element_type=F32)


def tn(a, b):
    return lax.dot_general(a, b, (((0,), (0,)), ((), ())), preferred_element_type=F32)


HOME = (3, 3)
MOVED = ((3, 3, 2), (4, 4, 4))
CHUNKS = tuple(HOME + moved for moved in MOVED)
COUNT = tuple(sum(sizes) for sizes in CHUNKS)
ORDER = ('M', 'N0', 'N1', 'O', 'T0', 'T1', 'g', 'F0', 'N2', 'C0', 'F1', 'N3', 'C1', 'N4', 'F2', 'D0', 'P0', 'Q0', 'P2', 'C2', 'G2', 'D1', 'P1', 'Q1', 'F3', 'P3', 'C3', 'G3', 'F4', 'P4', 'D2', 'Q2', 'C4', 'G4', 'D3', 'Q3', 'D4', 'Q4')
END_ORDER = ('L0', 'L1', 'B', 'L2', 'R2', 'L3', 'R3', 'L4', 'R4')
WHOLE = tuple(c for c in range(len(CHUNKS[0])) if f"G{c}" not in ORDER)


def kernel(
    n_p, n_q, x_hbm, lw_hbm, rw_hbm, lg_hbm, rg_hbm, gain_hbm, ow_hbm, og_hbm, out_ref,
    x_ref, w_ref, gain_ref, x_s, w_s, gain_s,
    turn, lsend, rsend, lbuf, rbuf, osend, orecv, gate,
    a_ss, a_rs, b_rs, f_ss, own_rs, f_rs, e_ss, o_ss, o_rs,
):
    p = lax.axis_index("pr")
    q = lax.axis_index("pc")
    half = q // 2
    mid, end = 1 + half, 3 * half
    far_mid, far_end = 2 - half, 3 - 3 * half
    at_mid = q == mid
    width = x_ref.shape[1]
    rows = x_ref.shape[0] // 2
    channels = w_ref.shape[2]
    count = n_p * x_ref.shape[0]
    planes = (mid, end, far_mid, far_end)
    n_c = len(CHUNKS[0])
    n_h = len(HOME)
    n_home = sum(HOME)
    parts = [
        [pl.ds(sum(sizes[:c]) * SUB, sizes[c] * SUB) for c in range(n_c)] for sizes in CHUNKS
    ]
    wholes = [pl.ds(0, n * SUB) for n in COUNT]
    moveds = [pl.ds(n_home * SUB, (n - n_home) * SUB) for n in COUNT]
    home = pl.ds(0, n_home * SUB)
    others = pl.ds(1, n_p - 1)
    pair = pl.ds(0, 2)
    away = pl.ds(2, n_p - 2)
    core = lax.rem(p, 2)

    def by_core(act):
        for k in range(2):

            @pl.when(core == k)
            def _():
                act(k)

    bring_x = pltpu.make_async_copy(x_hbm, x_ref, x_s)
    bring_gain = pltpu.make_async_copy(gain_hbm, gain_ref, gain_s)
    bring_x.start()
    for at, src in enumerate((lw_hbm, lg_hbm, rw_hbm, rg_hbm, og_hbm, ow_hbm)):
        pltpu.make_async_copy(src, w_ref.at[at], w_s).start()
    bring_gain.start()

    barrier = pltpu.get_barrier_semaphore()
    def greet(to):
        pl.semaphore_signal(barrier, inc=1, device_id=to, device_id_type=MESH)

    for dp in range(1, n_p):
        greet((p ^ dp, q))

    @pl.when(at_mid)
    def _():
        greet((p, far_mid))
        greet((p, end))


    def pair_rows(k):
        return jnp.concatenate([x_ref[k], x_ref[k + rows]], axis=0)

    def factor(first, send):
        both = jnp.concatenate([w_ref[first].T, w_ref[first + 1].T], axis=0)

        def step(k, _):
            pr = nt(both, pair_rows(k))
            turn[pl.ds(k, channels, stride=STEP), :] = pr[:channels] * jax.nn.sigmoid(pr[channels:])
            return 0

        lax.fori_loop(0, rows, step, 0, unroll=UF)

        def cast(e, _):
            for k in range(2):
                for d in range(COUNT[k]):
                    at = (e * sum(COUNT) + k * COUNT[0] + d) * STEP
                    send[e * 2 + k, d * SUB : (d + 1) * SUB] = turn[pl.ds(at, SUB), :].astype(BF16)
            return 0

        lax.fori_loop(0, n_p // 2, cast, 0)

    def remote(src, dst, send_sem, recv_sem, to):
        return pltpu.make_async_remote_copy(
            src_ref=src, dst_ref=dst, send_sem=send_sem, recv_sem=recv_sem,
            device_id=to, device_id_type=MESH,
        )

    def arrived(ref, sem):
        remote(ref, ref, sem, sem, (p, q)).wait_recv()

    def left(ref, sem):
        remote(ref, ref, sem, sem, (p, q)).wait_send()

    def spread(k, sems, send, buf, pieces):
        def give(dp, lines, sem):
            remote(
                send.at[p ^ dp, lines], buf.at[0, dp, lines],
                a_ss.at[dp & 1], sem, (p ^ dp, q),
            ).start()

        n = len(pieces[0])
        give(1, wholes[1 - k], sems.at[n])
        for at in range(n):
            for dp in range(n_p - 1, 1, -1):
                give(dp, pieces[k ^ (dp & 1)][at], sems.at[at])

    def own(buf, slot_from, slot_to, at, to, slots, lines):
        remote(
            buf.at[slot_from, slots, lines], buf.at[slot_to, slots, lines],
            f_ss.at[at % 2], own_rs.at[at], to,
        ).start()

    def to_end(slot_from, slot_to, c):
        remote(
            lbuf.at[slot_from, :, parts[0][c]], lbuf.at[slot_to, :, parts[0][c]],
            e_ss, f_rs.at[slot_to, c], (p, end),
        ).start()

    pltpu.make_async_copy(w_ref, w_ref, w_s).wait()
    bring_gain.wait()
    bring_x.wait()
    factor(0, lsend)
    pl.semaphore_wait(barrier, n_p)

    def send_left(k):
        lines = wholes[k]
        lbuf[0, 0, lines] = lsend[p, lines]

        @pl.when(at_mid)
        def _():
            own(lbuf, 0, 2, 2, (p, far_mid), 0, lines)

        @pl.when(jnp.logical_not(at_mid))
        def _():
            own(lbuf, 0, 1, 0, (p, mid), 0, lines)

        spread(k, a_rs, lsend, lbuf, parts)

    by_core(send_left)
    factor(2, rsend)

    def make_gate(k, _):
        gate[k] = jax.nn.sigmoid(
            jnp.dot(pair_rows(k), w_ref[4], preferred_element_type=F32)
        )
        return 0

    def gates():
        lax.fori_loop(0, rows, make_gate, 0, unroll=4)

    low = lax.broadcasted_iota(jnp.int32, (SUB, LANES), 1) < width

    def pass_on_core(k):
        sizes, part, whole, moved = CHUNKS[k], parts[k], wholes[k], moveds[k]

        rbuf[0, 0, whole] = rsend[p, whole]
        spread(k, b_rs, rsend, rbuf, [(*parts[n][n_h:], home) for n in range(2)])

        def pass_on(buf, slot_from, slot_to, at, c, to):
            remote(
                buf.at[slot_from, away, part[c]], buf.at[slot_to, away, part[c]],
                f_ss.at[at % 2], f_rs.at[at, c], to,
            ).start()

        def multiply(g, c, plane, sides):
            first = sum(sizes[:c])
            done = o_rs.at[0 if c < n_h else 1 + k]

            def some(these):
                def products(d, _):
                    at = pl.ds(pl.multiple_of(d * SUB, SUB), SUB)
                    lines = lbuf[g, :, at, :].reshape(n_p * SUB, LANES)
                    right = [rbuf[j, :, at, :].reshape(n_p * SUB, LANES) for j in these]
                    sums = tn(lines, right[0] if len(these) == 1 else jnp.concatenate(right, axis=1))
                    for n, j in enumerate(these):
                        acc = sums[:, n * LANES : (n + 1) * LANES]
                        for b in range(2):
                            top = b * 2 * SUB
                            a0, c0 = acc[top : top + SUB], acc[top + SUB : top + 2 * SUB]
                            b0 = acc[width + top : width + top + SUB]
                            d0 = acc[width + top + SUB : width + top + 2 * SUB]
                            tile = jnp.where(low, a0, d0) + pltpu.roll(
                                jnp.where(low, c0, b0), width, 1
                            )
                            osend[g, b, j, at, :] = (tile * count ** (-0.5)).astype(BF16)
                    return 0

                lax.fori_loop(first, first + sizes[c], products, 0, unroll=sizes[c])

            def give_end():
                for b in range(2):
                    remote(
                        osend.at[g, b, 1, part[c]], orecv.at[p, part[c]],
                        o_ss.at[1], done, (plane * 2 + b, end),
                    ).start()

            if sides == 2 and c == n_c - 1:
                some((1,))
                give_end()
                some((0,))
            else:
                some(tuple(range(sides)))
                if sides == 2:
                    give_end()
            for b in range(2):
                to_p = plane * 2 + b

                @pl.when(to_p != p)
                def _():
                    remote(
                        osend.at[g, b, 0, part[c]], orecv.at[p, part[c]],
                        o_ss.at[0], done, (to_p, q),
                    ).start()

                @pl.when(to_p == p)
                def _():
                    orecv[p, part[c]] = osend[g, b, 0, part[c]]

        turn_of = p // 2

        def rotated(n, c, plane_of, sides):
            for t in range(n):
                g = lax.rem(turn_of + t, n)
                plane = plane_of[n - 1]
                for at in range(n - 1):
                    plane = jnp.where(g == at, plane_of[at], plane)
                multiply(g, c, plane, sides)

        @pl.when(jnp.logical_not(at_mid))
        def _():
            def pass_left(c):
                arrived(lbuf.at[0, away, part[c]], a_rs.at[c])
                pass_on(lbuf, 0, 1, 0, c, (p, mid))

            def pass_right(c):
                arrived(rbuf.at[0, away, part[c]], b_rs.at[c - n_h])
                pass_on(rbuf, 0, 1, 1, c, (p, mid))

            arrived(lbuf.at[0, 1, whole], a_rs.at[n_c])
            own(lbuf, 0, 1, 0, (p, mid), 1, whole)

            def right_pair():
                arrived(rbuf.at[0, 1, whole], b_rs.at[n_c - n_h + 1])
                own(rbuf, 0, 1, 1, (p, mid), pair, moved)

            for step in END_ORDER:
                if step == "B":
                    right_pair()
                else:
                    {"L": pass_left, "R": pass_right}[step[0]](int(step[1:]))
            gates()
            for c in range(n_h):
                if c == 0:
                    arrived(rbuf.at[0, away, home], b_rs.at[n_c - n_h])
                arrived(lbuf.at[1, :, part[c]], f_rs.at[1, c])
                arrived(lbuf.at[2, :, part[c]], f_rs.at[2, c])
                rotated(3, c, (end, mid, far_mid), 1)
            for c in range(n_h):
                arrived(lbuf.at[3, :, part[c]], f_rs.at[3, c])
                multiply(3, c, far_end, 1)
            left(lbuf.at[0, :, whole], f_ss.at[0])
            left(lbuf.at[0, :, moved], f_ss.at[1])

        @pl.when(at_mid)
        def _():
            def pass_near(c):
                arrived(lbuf.at[0, away, part[c]], a_rs.at[c])
                pass_on(lbuf, 0, 2, 2, c, (p, far_mid))

            def pass_far(c):
                arrived(lbuf.at[1, away, part[c]], f_rs.at[0, c])
                pass_on(lbuf, 1, 3, 3, c, (p, far_mid))

            def came(c):
                if c == 0:
                    arrived(lbuf.at[2, pair, whole], own_rs.at[2])
                arrived(lbuf.at[2, away, part[c]], f_rs.at[2, c])
                if c < n_h:
                    to_end(2, 2, c)

            def near(c):
                if c == n_h:
                    arrived(rbuf.at[1, pair, moved], own_rs.at[1])
                if c == 0:
                    arrived(rbuf.at[0, away, home], b_rs.at[n_c - n_h])
                if c >= n_h:
                    arrived(rbuf.at[0, away, part[c]], b_rs.at[c - n_h])
                    arrived(rbuf.at[1, away, part[c]], f_rs.at[1, c])
                rotated(3 if c in WHOLE else 2, c, planes, 1 if c < n_h else 2)

            def near_to_end(c):
                to_end(0, 1, c)

            def far_near(c):
                multiply(2, c, far_mid, 1 if c < n_h else 2)

            def mate():
                arrived(lbuf.at[0, 1, whole], a_rs.at[n_c])
                own(lbuf, 0, 2, 2, (p, far_mid), 1, whole)

            def onward():
                arrived(lbuf.at[1, pair, whole], own_rs.at[0])
                own(lbuf, 1, 3, 3, (p, far_mid), pair, whole)

            def came_far(c):
                if c == 0:
                    arrived(lbuf.at[3, pair, whole], own_rs.at[3])
                arrived(lbuf.at[3, away, part[c]], f_rs.at[3, c])
                if c < n_h:
                    to_end(3, 3, c)

            def last(c):
                multiply(3, c, far_end, 1 if c < n_h else 2)

            first_right = next(step for step in ORDER if step[0] == "P")
            act = {"N": pass_near, "F": pass_far, "C": came, "P": near, "G": far_near, "T": near_to_end, "D": came_far, "Q": last}
            alone = {"M": mate, "O": onward, "g": gates}
            for step in ORDER:
                if step == first_right:
                    arrived(rbuf.at[0, 1, whole], b_rs.at[n_c - n_h + 1])
                if step in alone:
                    alone[step]()
                else:
                    act[step[0]](int(step[1:]))
            left(lbuf.at[0, :, whole], f_ss.at[0])
            left(lbuf.at[0, :, whole], f_ss.at[1])
            left(lbuf.at[pl.ds(1, 3), :, home], e_ss)

    by_core(pass_on_core)
    gain = jnp.broadcast_to(gain_ref[...], (channels, channels)).T

    def close(k):
        left(lbuf.at[pl.ds(0, 2), pl.ds(0, n_p // 2 - 1), wholes[k]], a_ss.at[0])
        left(lbuf.at[pl.ds(0, 2), pl.ds(0, n_p // 2), wholes[1 - k]], a_ss.at[1])
        arrived(orecv.at[others, home], o_rs.at[0])
        arrived(orecv.at[pl.ds(0, n_p // 2), moveds[1 - k]], o_rs.at[2 - k])

        @pl.when(at_mid)
        def _():
            arrived(orecv.at[pl.ds(0, n_p // 2 - 1), moveds[k]], o_rs.at[1 + k])

        @pl.when(jnp.logical_not(at_mid))
        def _():
            arrived(orecv.at[pl.ds(0, n_p // 2), moveds[k]], o_rs.at[1 + k])

    by_core(close)

    def widen(e, _):
        for k in range(2):
            for d in range(COUNT[k]):
                at = (e * sum(COUNT) + k * COUNT[0] + d) * STEP
                turn[pl.ds(at, SUB), :] = orecv[e * 2 + k, d * SUB : (d + 1) * SUB].astype(F32)
        return 0

    lax.fori_loop(0, n_p // 2, widen, 0)

    def finish(k, _):
        v = turn[pl.ds(k, channels, stride=STEP), :]
        v = v - jnp.mean(v, axis=0, keepdims=True)
        v = v * lax.rsqrt(jnp.mean(v * v, axis=0, keepdims=True) + 1e-05) * gain
        res = (tn(v.astype(BF16), w_ref[5]) * gate[k]).astype(BF16)
        out_ref[k] = res[:width]
        out_ref[k + rows] = res[width:]
        return 0

    lax.fori_loop(0, rows, finish, 0, unroll=UE)

    left(orecv.at[others, home], o_ss.at[0])

    def leave(k):
        left(orecv.at[others, moveds[k]], o_ss.at[0])
        left(orecv.at[:, moveds[k]], o_ss.at[1])

    @pl.when(at_mid)
    def _():
        by_core(leave)


def fused(n_p, n_q, pair_array, lw, rw, lg, rg, gain, ow, og):
    channels = lw.shape[1]
    slab = max(COUNT) * SUB
    rows = pair_array.shape[0] // 2
    dma = pltpu.SemaphoreType.DMA
    return pl.pallas_call(
        functools.partial(kernel, n_p, n_q),
        out_shape=pltpu.VMEM(pair_array.shape, BF16),
        in_specs=[pl.BlockSpec(memory_space=pltpu.HBM)] * 8,
        out_specs=pl.BlockSpec(memory_space=pltpu.VMEM),
        scratch_shapes=[
            pltpu.VMEM(pair_array.shape, BF16),
            pltpu.VMEM((6, *lw.shape), BF16),
            pltpu.VMEM((1, channels), F32),
            dma(()),
            dma(()),
            dma(()),
            pltpu.VMEM((channels * STEP, LANES), F32),
            pltpu.VMEM((n_p, slab, LANES), BF16),
            pltpu.VMEM((n_p, slab, LANES), BF16),
            pltpu.VMEM((4, n_p, slab, LANES), BF16),
            pltpu.VMEM((2, n_p, slab, LANES), BF16),
            pltpu.VMEM((4, 2, 2, slab, LANES), BF16),
            pltpu.VMEM((n_p, slab, LANES), BF16),
            pltpu.VMEM((rows, LANES, channels), F32),
            dma((2,)),
            dma((len(CHUNKS[0]) + 1,)),
            dma((len(MOVED[0]) + 2,)),
            dma((2,)),
            dma((4,)),
            dma((4, len(CHUNKS[0]))),
            dma(()),
            dma((2,)),
            dma((3,)),
        ],
        compiler_params=pltpu.CompilerParams(
            collective_id=0, has_side_effects=True, vmem_limit_bytes=33_554_432
        ),
    )(*(
        pltpu.with_memory_space_constraint(a, pltpu.HBM)
        for a in (pair_array, lw, rw, lg, rg, gain.reshape(1, channels), ow, og)
    ))


def solution(mesh):
    n_p, n_q = mesh.shape["pr"], mesh.shape["pc"]

    def on_device(pair_array, lw, *rest):
        first, second, wide = pair_array.shape
        fits = (
            n_q == 4
            and first == 2 * SUB
            and second == 2 * first
            and n_p == 2 * n_q
            and 2 * second == LANES
            and wide == LANES
            and lw.shape[1] == LANES
            and n_p // 2 * sum(COUNT) == LANES
        )
        if fits:
            return fused(n_p, n_q, pair_array, lw, *rest)
        return plain(pair_array, lw, *rest)

    return jax.shard_map(
        on_device,
        mesh=mesh,
        in_specs=(P("pr", "pc", None), P(), P(), P(), P(), P(), P(), P()),
        out_specs=P("pr", "pc", None),
        check_vma=False,
    )
```

```python
import functools

import jax
import jax.numpy as jnp
from jax import lax
from jax.experimental import pallas as pl
from jax.experimental.pallas import tpu as pltpu
from jax.sharding import PartitionSpec as P

MESH = pl.DeviceIdType.MESH
BF16 = jnp.bfloat16
F32 = jnp.float32
LANES = 128
SUB = 16
STEP = 17
UF, UP, UE = 16, 8, 16


def unit_channels(values, channel_gain):
    centred = values - jnp.mean(values, axis=-1, keepdims=True)
    return (
        centred
        * lax.rsqrt(jnp.mean(centred * centred, axis=-1, keepdims=True) + 1e-05)
        * channel_gain
    )


def make_factors(pair_in, left_weight, right_weight, left_gate, right_gate):
    left = jnp.einsum("ijc,cd->ijd", pair_in, left_weight, preferred_element_type=F32)
    left = left * jax.nn.sigmoid(
        jnp.einsum("ijc,cd->ijd", pair_in, left_gate, preferred_element_type=F32)
    )
    right = jnp.einsum("ijc,cd->ijd", pair_in, right_weight, preferred_element_type=F32)
    right = right * jax.nn.sigmoid(
        jnp.einsum("ijc,cd->ijd", pair_in, right_gate, preferred_element_type=F32)
    )
    return (pair_in, left.astype(BF16), right.astype(BF16))


def to_pair(mixed, ready, mid_gain, out_weight, out_gate):
    scaled = unit_channels(mixed.astype(F32), mid_gain).astype(BF16)
    scaled = lax.optimization_barrier(scaled)
    gate = jax.nn.sigmoid(jnp.einsum("ijc,cd->ijd", ready, out_gate, preferred_element_type=F32))
    return (
        jnp.einsum("ijd,dc->ijc", scaled, out_weight, preferred_element_type=F32) * gate
    ).astype(BF16)


def plain(
    pair_array, left_weight, right_weight, left_gate, right_gate, mid_gain, out_weight, out_gate
):
    ready, left, right = make_factors(pair_array, left_weight, right_weight, left_gate, right_gate)
    count = pair_array.shape[0] * lax.axis_size("pr")
    left_lines, right_lines = (
        lax.all_to_all(left, "pr", split_axis=2, concat_axis=0, tiled=True),
        lax.all_to_all(right, "pr", split_axis=2, concat_axis=0, tiled=True),
    )
    strip = jnp.einsum(
        "kid,kjd->ijd",
        lax.all_gather(left_lines, "pc", axis=1, tiled=True),
        right_lines,
        preferred_element_type=F32,
    )
    strip = (strip * count ** (-0.5)).astype(BF16)
    mixed = lax.all_to_all(strip, "pr", split_axis=0, concat_axis=2, tiled=True)
    return to_pair(mixed, ready, mid_gain, out_weight, out_gate)


def nt(a, b):
    return lax.dot_general(a, b, (((1,), (1,)), ((), ())), preferred_element_type=F32)


def tn(a, b):
    return lax.dot_general(a, b, (((0,), (0,)), ((), ())), preferred_element_type=F32)


HOME = (3, 3)
MOVED = (4, 3)
CHUNKS = (HOME + (3, 3, 1), HOME + (5, 4, 4))
COUNT = tuple(sum(sizes) for sizes in CHUNKS)
ORDER = ('M', 'N0', 'N1', 'O', 'T0', 'T1', 'g', 'F0', 'N2', 'C0', 'F1', 'N3', 'C1', 'N4', 'F2', 'D0', 'P0', 'Q0', 'P2', 'C2', 'G2', 'D1', 'P1', 'Q1', 'F3', 'P3', 'C3', 'G3', 'F4', 'P4', 'D2', 'Q2', 'C4', 'G4', 'D3', 'Q3', 'D4', 'Q4')
END_ORDER = ('L0', 'L1', 'B', 'L2', 'R2', 'L3', 'R3', 'L4', 'R4')
WHOLE = tuple(c for c in range(len(CHUNKS[0])) if f"G{c}" not in ORDER)


def kernel(
    n_p, n_q, x_hbm, lw_hbm, rw_hbm, lg_hbm, rg_hbm, gain_hbm, ow_hbm, og_hbm, out_ref,
    x_ref, w_ref, gain_ref, x_s, w_s, gain_s,
    turn, lsend, rsend, lbuf, rbuf, osend, orecv, gate,
    a_ss, a_rs, b_rs, f_ss, own_rs, f_rs, e_ss, o_ss, o_rs,
):
    p = lax.axis_index("pr")
    q = lax.axis_index("pc")
    half = q // 2
    mid, end = 1 + half, 3 * half
    far_mid, far_end = 2 - half, 3 - 3 * half
    at_mid = q == mid
    width = x_ref.shape[1]
    rows = x_ref.shape[0] // 2
    channels = w_ref.shape[2]
    count = n_p * x_ref.shape[0]
    planes = (mid, end, far_mid, far_end)
    n_c = len(CHUNKS[0])
    n_h = len(HOME)
    n_home = sum(HOME)
    parts = [
        [pl.ds(sum(sizes[:c]) * SUB, sizes[c] * SUB) for c in range(n_c)] for sizes in CHUNKS
    ]
    wholes = [pl.ds(0, n * SUB) for n in COUNT]
    moveds = [pl.ds(n_home * SUB, (n - n_home) * SUB) for n in COUNT]
    home = pl.ds(0, n_home * SUB)
    others = pl.ds(1, n_p - 1)
    pair = pl.ds(0, 2)
    away = pl.ds(2, n_p - 2)
    core = lax.rem(p, 2)

    def by_core(act):
        for k in range(2):

            @pl.when(core == k)
            def _():
                act(k)

    bring_x = pltpu.make_async_copy(x_hbm, x_ref, x_s)
    bring_gain = pltpu.make_async_copy(gain_hbm, gain_ref, gain_s)
    bring_x.start()
    for at, src in enumerate((lw_hbm, lg_hbm, rw_hbm, rg_hbm, og_hbm, ow_hbm)):
        pltpu.make_async_copy(src, w_ref.at[at], w_s).start()
    bring_gain.start()

    barrier = pltpu.get_barrier_semaphore()
    def greet(to):
        pl.semaphore_signal(barrier, inc=1, device_id=to, device_id_type=MESH)

    for dp in range(1, n_p):
        greet((p ^ dp, q))

    @pl.when(at_mid)
    def _():
        greet((p, far_mid))
        greet((p, end))


    def pair_rows(k):
        return jnp.concatenate([x_ref[k], x_ref[k + rows]], axis=0)

    def factor(first, send):
        both = jnp.concatenate([w_ref[first].T, w_ref[first + 1].T], axis=0)

        def step(k, _):
            pr = nt(both, pair_rows(k))
            turn[pl.ds(k, channels, stride=STEP), :] = pr[:channels] * jax.nn.sigmoid(pr[channels:])
            return 0

        lax.fori_loop(0, rows, step, 0, unroll=UF)

        def cast(e, _):
            for k in range(2):
                for d in range(COUNT[k]):
                    at = (e * sum(COUNT) + k * COUNT[0] + d) * STEP
                    send[e * 2 + k, d * SUB : (d + 1) * SUB] = turn[pl.ds(at, SUB), :].astype(BF16)
            return 0

        lax.fori_loop(0, n_p // 2, cast, 0)

    def remote(src, dst, send_sem, recv_sem, to):
        return pltpu.make_async_remote_copy(
            src_ref=src, dst_ref=dst, send_sem=send_sem, recv_sem=recv_sem,
            device_id=to, device_id_type=MESH,
        )

    def arrived(ref, sem):
        remote(ref, ref, sem, sem, (p, q)).wait_recv()

    def left(ref, sem):
        remote(ref, ref, sem, sem, (p, q)).wait_send()

    def spread(k, sems, send, buf, pieces):
        def give(dp, lines, sem):
            remote(
                send.at[p ^ dp, lines], buf.at[0, dp, lines],
                a_ss.at[dp & 1], sem, (p ^ dp, q),
            ).start()

        n = len(pieces[0])
        give(1, wholes[1 - k], sems.at[n])
        for at in range(n):
            for dp in range(n_p - 1, 1, -1):
                give(dp, pieces[k ^ (dp & 1)][at], sems.at[at])

    def own(buf, slot_from, slot_to, at, to, slots, lines):
        remote(
            buf.at[slot_from, slots, lines], buf.at[slot_to, slots, lines],
            f_ss.at[at % 2], own_rs.at[at], to,
        ).start()

    def to_end(slot_from, slot_to, c):
        remote(
            lbuf.at[slot_from, :, parts[0][c]], lbuf.at[slot_to, :, parts[0][c]],
            e_ss, f_rs.at[slot_to, c], (p, end),
        ).start()

    pltpu.make_async_copy(w_ref, w_ref, w_s).wait()
    bring_gain.wait()
    bring_x.wait()
    factor(0, lsend)
    pl.semaphore_wait(barrier, n_p)

    def send_left(k):
        lines = wholes[k]
        lbuf[0, 0, lines] = lsend[p, lines]

        @pl.when(at_mid)
        def _():
            own(lbuf, 0, 2, 2, (p, far_mid), 0, lines)

        @pl.when(jnp.logical_not(at_mid))
        def _():
            own(lbuf, 0, 1, 0, (p, mid), 0, lines)

        spread(k, a_rs, lsend, lbuf, parts)

    by_core(send_left)
    factor(2, rsend)

    def make_gate(k, _):
        gate[k] = jax.nn.sigmoid(
            jnp.dot(pair_rows(k), w_ref[4], preferred_element_type=F32)
        )
        return 0

    def gates():
        lax.fori_loop(0, rows, make_gate, 0, unroll=4)

    low = lax.broadcasted_iota(jnp.int32, (SUB, LANES), 1) < width

    def pass_on_core(k):
        sizes, part, whole, moved = CHUNKS[k], parts[k], wholes[k], moveds[k]

        rbuf[0, 0, whole] = rsend[p, whole]
        spread(k, b_rs, rsend, rbuf, [(*parts[n][n_h:], home) for n in range(2)])

        def pass_on(buf, slot_from, slot_to, at, c, to):
            remote(
                buf.at[slot_from, away, part[c]], buf.at[slot_to, away, part[c]],
                f_ss.at[at % 2], f_rs.at[at, c], to,
            ).start()

        def multiply(g, c, plane, sides):
            first = sum(sizes[:c])
            done = o_rs.at[0 if c < n_h else 1 + k]

            def some(these):
                def products(d, _):
                    at = pl.ds(pl.multiple_of(d * SUB, SUB), SUB)
                    lines = lbuf[g, :, at, :].reshape(n_p * SUB, LANES)
                    right = [rbuf[j, :, at, :].reshape(n_p * SUB, LANES) for j in these]
                    sums = tn(lines, right[0] if len(these) == 1 else jnp.concatenate(right, axis=1))
                    for n, j in enumerate(these):
                        acc = sums[:, n * LANES : (n + 1) * LANES]
                        for b in range(2):
                            top = b * 2 * SUB
                            a0, c0 = acc[top : top + SUB], acc[top + SUB : top + 2 * SUB]
                            b0 = acc[width + top : width + top + SUB]
                            d0 = acc[width + top + SUB : width + top + 2 * SUB]
                            tile = jnp.where(low, a0, d0) + pltpu.roll(
                                jnp.where(low, c0, b0), width, 1
                            )
                            osend[g, b, j, at, :] = (tile * count ** (-0.5)).astype(BF16)
                    return 0

                lax.fori_loop(first, first + sizes[c], products, 0, unroll=sizes[c])

            def give_end():
                for b in range(2):
                    remote(
                        osend.at[g, b, 1, part[c]], orecv.at[p, part[c]],
                        o_ss.at[1], done, (plane * 2 + b, end),
                    ).start()

            if sides == 2 and c == n_c - 1:
                some((1,))
                give_end()
                some((0,))
            else:
                some(tuple(range(sides)))
                if sides == 2:
                    give_end()
            for b in range(2):
                to_p = plane * 2 + b

                @pl.when(to_p != p)
                def _():
                    remote(
                        osend.at[g, b, 0, part[c]], orecv.at[p, part[c]],
                        o_ss.at[0], done, (to_p, q),
                    ).start()

                @pl.when(to_p == p)
                def _():
                    orecv[p, part[c]] = osend[g, b, 0, part[c]]

        turn_of = p // 2

        def rotated(n, c, plane_of, sides):
            for t in range(n):
                g = lax.rem(turn_of + t, n)
                plane = plane_of[n - 1]
                for at in range(n - 1):
                    plane = jnp.where(g == at, plane_of[at], plane)
                multiply(g, c, plane, sides)

        @pl.when(jnp.logical_not(at_mid))
        def _():
            def pass_left(c):
                arrived(lbuf.at[0, away, part[c]], a_rs.at[c])
                pass_on(lbuf, 0, 1, 0, c, (p, mid))

            def pass_right(c):
                arrived(rbuf.at[0, away, part[c]], b_rs.at[c - n_h])
                pass_on(rbuf, 0, 1, 1, c, (p, mid))

            arrived(lbuf.at[0, 1, whole], a_rs.at[n_c])
            own(lbuf, 0, 1, 0, (p, mid), 1, whole)

            def right_pair():
                arrived(rbuf.at[0, 1, whole], b_rs.at[n_c - n_h + 1])
                own(rbuf, 0, 1, 1, (p, mid), pair, moved)

            for step in END_ORDER:
                if step == "B":
                    right_pair()
                else:
                    {"L": pass_left, "R": pass_right}[step[0]](int(step[1:]))
            gates()
            for c in range(n_h):
                if c == 0:
                    arrived(rbuf.at[0, away, home], b_rs.at[n_c - n_h])
                arrived(lbuf.at[1, :, part[c]], f_rs.at[1, c])
                arrived(lbuf.at[2, :, part[c]], f_rs.at[2, c])
                rotated(3, c, (end, mid, far_mid), 1)
            for c in range(n_h):
                arrived(lbuf.at[3, :, part[c]], f_rs.at[3, c])
                multiply(3, c, far_end, 1)
            left(lbuf.at[0, :, whole], f_ss.at[0])
            left(lbuf.at[0, :, moved], f_ss.at[1])

        @pl.when(at_mid)
        def _():
            def pass_near(c):
                arrived(lbuf.at[0, away, part[c]], a_rs.at[c])
                pass_on(lbuf, 0, 2, 2, c, (p, far_mid))

            def pass_far(c):
                arrived(lbuf.at[1, away, part[c]], f_rs.at[0, c])
                pass_on(lbuf, 1, 3, 3, c, (p, far_mid))

            def came(c):
                if c == 0:
                    arrived(lbuf.at[2, pair, whole], own_rs.at[2])
                arrived(lbuf.at[2, away, part[c]], f_rs.at[2, c])
                if c < n_h:
                    to_end(2, 2, c)

            def near(c):
                if c == n_h:
                    arrived(rbuf.at[1, pair, moved], own_rs.at[1])
                if c == 0:
                    arrived(rbuf.at[0, away, home], b_rs.at[n_c - n_h])
                if c >= n_h:
                    arrived(rbuf.at[0, away, part[c]], b_rs.at[c - n_h])
                    arrived(rbuf.at[1, away, part[c]], f_rs.at[1, c])
                rotated(3 if c in WHOLE else 2, c, planes, 1 if c < n_h else 2)

            def near_to_end(c):
                to_end(0, 1, c)

            def far_near(c):
                multiply(2, c, far_mid, 1 if c < n_h else 2)

            def mate():
                arrived(lbuf.at[0, 1, whole], a_rs.at[n_c])
                own(lbuf, 0, 2, 2, (p, far_mid), 1, whole)

            def onward():
                arrived(lbuf.at[1, pair, whole], own_rs.at[0])
                own(lbuf, 1, 3, 3, (p, far_mid), pair, whole)

            def came_far(c):
                if c == 0:
                    arrived(lbuf.at[3, pair, whole], own_rs.at[3])
                arrived(lbuf.at[3, away, part[c]], f_rs.at[3, c])
                if c < n_h:
                    to_end(3, 3, c)

            def last(c):
                multiply(3, c, far_end, 1 if c < n_h else 2)

            first_right = next(step for step in ORDER if step[0] == "P")
            act = {"N": pass_near, "F": pass_far, "C": came, "P": near, "G": far_near, "T": near_to_end, "D": came_far, "Q": last}
            alone = {"M": mate, "O": onward, "g": gates}
            for step in ORDER:
                if step == first_right:
                    arrived(rbuf.at[0, 1, whole], b_rs.at[n_c - n_h + 1])
                if step in alone:
                    alone[step]()
                else:
                    act[step[0]](int(step[1:]))
            left(lbuf.at[0, :, whole], f_ss.at[0])
            left(lbuf.at[0, :, whole], f_ss.at[1])
            left(lbuf.at[pl.ds(1, 3), :, home], e_ss)

    by_core(pass_on_core)
    gain = jnp.broadcast_to(gain_ref[...], (channels, channels)).T

    def close(k):
        left(lbuf.at[pl.ds(0, 2), pl.ds(0, n_p // 2 - 1), wholes[k]], a_ss.at[0])
        left(lbuf.at[pl.ds(0, 2), pl.ds(0, n_p // 2), wholes[1 - k]], a_ss.at[1])
        arrived(orecv.at[others, home], o_rs.at[0])
        arrived(orecv.at[pl.ds(0, n_p // 2), moveds[1 - k]], o_rs.at[2 - k])

        @pl.when(at_mid)
        def _():
            arrived(orecv.at[pl.ds(0, n_p // 2 - 1), moveds[k]], o_rs.at[1 + k])

        @pl.when(jnp.logical_not(at_mid))
        def _():
            arrived(orecv.at[pl.ds(0, n_p // 2), moveds[k]], o_rs.at[1 + k])

    by_core(close)

    def widen(e, _):
        for k in range(2):
            for d in range(COUNT[k]):
                at = (e * sum(COUNT) + k * COUNT[0] + d) * STEP
                turn[pl.ds(at, SUB), :] = orecv[e * 2 + k, d * SUB : (d + 1) * SUB].astype(F32)
        return 0

    lax.fori_loop(0, n_p // 2, widen, 0)

    def finish(k, _):
        v = turn[pl.ds(k, channels, stride=STEP), :]
        v = v - jnp.mean(v, axis=0, keepdims=True)
        v = v * lax.rsqrt(jnp.mean(v * v, axis=0, keepdims=True) + 1e-05) * gain
        res = (tn(v.astype(BF16), w_ref[5]) * gate[k]).astype(BF16)
        out_ref[k] = res[:width]
        out_ref[k + rows] = res[width:]
        return 0

    lax.fori_loop(0, rows, finish, 0, unroll=UE)

    left(orecv.at[others, home], o_ss.at[0])

    def leave(k):
        left(orecv.at[others, moveds[k]], o_ss.at[0])
        left(orecv.at[:, moveds[k]], o_ss.at[1])

    @pl.when(at_mid)
    def _():
        by_core(leave)


def fused(n_p, n_q, pair_array, lw, rw, lg, rg, gain, ow, og):
    channels = lw.shape[1]
    slab = max(COUNT) * SUB
    rows = pair_array.shape[0] // 2
    dma = pltpu.SemaphoreType.DMA
    return pl.pallas_call(
        functools.partial(kernel, n_p, n_q),
        out_shape=pltpu.VMEM(pair_array.shape, BF16),
        in_specs=[pl.BlockSpec(memory_space=pltpu.HBM)] * 8,
        out_specs=pl.BlockSpec(memory_space=pltpu.VMEM),
        scratch_shapes=[
            pltpu.VMEM(pair_array.shape, BF16),
            pltpu.VMEM((6, *lw.shape), BF16),
            pltpu.VMEM((1, channels), F32),
            dma(()),
            dma(()),
            dma(()),
            pltpu.VMEM((channels * STEP, LANES), F32),
            pltpu.VMEM((n_p, slab, LANES), BF16),
            pltpu.VMEM((n_p, slab, LANES), BF16),
            pltpu.VMEM((4, n_p, slab, LANES), BF16),
            pltpu.VMEM((2, n_p, slab, LANES), BF16),
            pltpu.VMEM((4, 2, 2, slab, LANES), BF16),
            pltpu.VMEM((n_p, slab, LANES), BF16),
            pltpu.VMEM((rows, LANES, channels), F32),
            dma((2,)),
            dma((len(CHUNKS[0]) + 1,)),
            dma((len(MOVED) + 3,)),
            dma((2,)),
            dma((4,)),
            dma((4, len(CHUNKS[0]))),
            dma(()),
            dma((2,)),
            dma((3,)),
        ],
        compiler_params=pltpu.CompilerParams(
            collective_id=0, has_side_effects=True, vmem_limit_bytes=33_554_432
        ),
    )(*(
        pltpu.with_memory_space_constraint(a, pltpu.HBM)
        for a in (pair_array, lw, rw, lg, rg, gain.reshape(1, channels), ow, og)
    ))


def solution(mesh):
    n_p, n_q = mesh.shape["pr"], mesh.shape["pc"]

    def on_device(pair_array, lw, *rest):
        first, second, wide = pair_array.shape
        fits = (
            n_q == 4
            and first == 2 * SUB
            and second == 2 * first
            and n_p == 2 * n_q
            and 2 * second == LANES
            and wide == LANES
            and lw.shape[1] == LANES
            and n_p // 2 * sum(COUNT) == LANES
        )
        if fits:
            return fused(n_p, n_q, pair_array, lw, *rest)
        return plain(pair_array, lw, *rest)

    return jax.shard_map(
        on_device,
        mesh=mesh,
        in_specs=(P("pr", "pc", None), P(), P(), P(), P(), P(), P(), P()),
        out_specs=P("pr", "pc", None),
        check_vma=False,
    )
```
